32 devices in a mesh: sub: 16 (over z, x, core), panel: 2 (over y).
Axes of the slice: x: 2, y: 2, z: 4, core: 2. Of those that a mesh axis runs over, the one named last changes fastest.
Arguments:
- solution: float32 [16384, 256], P('sub', 'panel'), may hold values from -6 to 6
- residual: float32 [16384, 256], P('sub', 'panel'), may hold values from -25 to 25
- shadow: float32 [16384, 256], P('sub', 'panel'), may hold values from -120 to 120
- direction: float32 [16384, 256], P('sub', 'panel'), may hold values from -6 to 6
- old_image: float32 [16384, 256], P('sub', 'panel'), may hold values from -6 to 6
- rho_prev: float32 [256], P('panel'), may hold values from 1 to 4
- alpha_prev: float32 [256], P('panel'), may hold values from 0.5 to 2
- omega_prev: float32 [256], P('panel'), may hold values from 0.5 to 2
- lower_inverse: bfloat16 [16, 1792, 1792], P('sub', None, 'panel'), may hold values from -0.4 to 0.4, as said below
- upper_inverse: bfloat16 [16, 1792, 1792], P('sub', None, 'panel'), may hold values from -0.4 to 0.4, as said below
- neighbours: int32 [16, 16384], P(None, 'sub'), may hold values from 0 to 1792, as said below
- edge_weight: float32 [16, 16384], P(None, 'sub'), may hold values from 0.1 to 1
- node_shift: float32 [16384], P('sub'), may hold values from 3 to 12
- send_rows: int32 [16, 2, 384], P('sub'), may hold values from 0 to 1023
Outputs:
- new_solution: float32 [16384, 256], P('sub', 'panel')
- new_residual: float32 [16384, 256], P('sub', 'panel')
- step_alpha: float32 [256], P('panel')
- step_omega: float32 [256], P('panel')
- next_rho: float32 [256], P('panel')
The draws below stay inside these ranges and needn't reach their ends.
Inputs may be any that keep to these rules, and one draw needn't show every extreme that they name: lower_inverse[s] is zero above its diagonal. upper_inverse[s] is zero below its diagonal. `neighbours`: an entry below 1024 is an owned node, from 1024 a ghost node from the lower neighbour's list, from 1408 one from the upper neighbour's list; 1792 marks an empty slot. send_rows[s, 0] lists the rows of subdomain s that subdomain s - 1 holds as ghosts, send_rows[s, 1] those that subdomain s + 1 holds, modulo 16.
All inputs are finite; a program needn't handle non-finite values.
Results may differ from the reference program's by a relative error of at most 0.0097.
Values may be sent and summed in bfloat16 or wider, within the bound.
No kernel may reach another device: no remote copies, remote signals or barrier semaphores. Data moves between devices by JAX's collectives and lax.ppermute only.
A program may use at most 64 MiB of HBM per device.

```python
import math
import jax
import jax.numpy as jnp
from jax import lax

OWN = 1024
SRC = 256
BORDER = 384
NB = 16
SUBS = 16
NODES = 16384
EXT = 1792


def residual_pair(key):
    base_key = jax.random.fold_in(key, 17)
    subkeys = jax.random.split(base_key, 4)
    position = lax.broadcasted_iota(jnp.float32, (NODES, 1), 0) / NODES
    rough_log = jax.random.uniform(subkeys[0], (NODES, 1), jnp.float32, -1.15, 1.15)
    row_scale = 0.5 * (1.0 + 2.0 * position) * jnp.exp(rough_log)
    values = jnp.clip(jax.random.normal(subkeys[1], (NODES, SRC), jnp.float32), -5.0, 5.0)
    noise_part = jnp.clip(jax.random.normal(subkeys[2], (NODES, SRC), jnp.float32), -5.0, 5.0)
    spread = jnp.exp(jax.random.uniform(subkeys[3], (1, SRC), jnp.float32, -1.2, 1.2))
    residual_part = row_scale * values
    return (residual_part, residual_part + spread * row_scale * noise_part)


def draw_residual(key, part):
    return residual_pair(key)[0]


def draw_shadow(key, part):
    return residual_pair(key)[1]


def triangle(key, below):
    subkeys = jax.random.split(key, 2)
    row_index = lax.broadcasted_iota(jnp.int32, (1, EXT, 1), 1)
    col_index = lax.broadcasted_iota(jnp.int32, (1, 1, EXT), 2)
    coupling = jnp.clip(jax.random.normal(subkeys[0], (SUBS, EXT, EXT), jnp.float32), -5.0, 5.0) * (0.4 / math.sqrt(EXT))
    diagonal = jax.random.uniform(subkeys[1], (SUBS, EXT, 1), jnp.float32, 0.7, 1.3)
    if below:
        keep_mask = row_index > col_index
    else:
        keep_mask = row_index < col_index
    return 0.3 * jnp.where(row_index == col_index, diagonal, jnp.where(keep_mask, coupling, 0.0))


def draw_lower_inverse(key, part):
    return triangle(jax.random.fold_in(key, 29), True).astype(jnp.bfloat16)


def draw_upper_inverse(key, part):
    return triangle(jax.random.fold_in(key, 31), False).astype(jnp.bfloat16)


def draw_neighbours(key, part):
    subkeys = jax.random.split(jax.random.fold_in(key, 41), 2)
    degree = jax.random.randint(subkeys[0], (1, NODES), NB - NB // 4, NB + 1)
    picked = jax.random.randint(subkeys[1], (NB, NODES), 0, EXT)
    slot_index = lax.broadcasted_iota(jnp.int32, (NB, NODES), 0)
    return jnp.where(slot_index < degree, picked, EXT).astype(jnp.int32)


def touch_ends(result, stream_key, least, largest):
    dims = result.shape
    spot = [jax.random.randint(jax.random.fold_in(stream_key, axis), (), 0, dims[axis]) for axis in range(len(dims))]
    result = result.at[tuple(spot)].set(least)
    longest = dims.index(max(dims))
    spot[longest] = (spot[longest] + 1) % dims[longest]
    return result.at[tuple(spot)].set(largest)


def levels(own_key, shape, cuts, smallest, high):
    gain = 1.0
    for axis_at, parts in cuts:
        heights = jax.random.uniform(jax.random.fold_in(jax.random.fold_in(own_key, 6), axis_at), (parts,), jnp.float32, smallest / len(cuts), high / len(cuts))
        gain = gain * jnp.repeat(jnp.exp(heights), shape[axis_at] // parts).reshape((-1,) + (1,) * (len(shape) - 1 - axis_at))
    return gain


def bell_draw(rng, shape, width, bound, cuts=(), dtype=jnp.bfloat16):
    drawn = jax.random.normal(rng, shape, jnp.float32) * width
    if len(cuts) > 0:
        drawn = levels(rng, shape, cuts, -0.22, 0.18) * drawn
    return jnp.clip(drawn, min=-bound, max=bound).astype(dtype)


def setup_inputs(seed: int = 0) -> dict:
    splits = jax.random.split(jax.random.key(seed), 15)
    return {
        "solution": bell_draw(splits[0], (NODES, SRC), 1.0, 6.0, ((0, 16), (1, 2)), jnp.float32),
        "residual": draw_residual(jax.random.fold_in(splits[14], 71), 0),
        "shadow": draw_shadow(jax.random.fold_in(splits[14], 71), 0),
        "direction": bell_draw(splits[3], (NODES, SRC), 1.0, 6.0, ((0, 16), (1, 2)), jnp.float32),
        "old_image": bell_draw(splits[4], (NODES, SRC), 1.0, 6.0, ((0, 16), (1, 2)), jnp.float32),
        "rho_prev": jnp.clip(jnp.exp(math.log(4.0) - 1.3862944 * jax.random.uniform(splits[5], (SRC,), jnp.float32) ** levels(splits[5], (SRC,), ((0, 2),), -0.2, 0.2)), 1.0, 4.0),
        "alpha_prev": jnp.clip(jnp.exp(math.log(2.0) - 1.3862944 * jax.random.uniform(splits[6], (SRC,), jnp.float32) ** levels(splits[6], (SRC,), ((0, 2),), -0.2, 0.2)), 0.5, 2.0),
        "omega_prev": jnp.clip(jnp.exp(math.log(2.0) - 1.3862944 * jax.random.uniform(splits[7], (SRC,), jnp.float32) ** levels(splits[7], (SRC,), ((0, 2),), -0.2, 0.2)), 0.5, 2.0),
        "lower_inverse": draw_lower_inverse(jax.random.fold_in(splits[14], 71), 0),
        "upper_inverse": draw_upper_inverse(jax.random.fold_in(splits[14], 71), 0),
        "neighbours": draw_neighbours(jax.random.fold_in(splits[14], 71), 0),
        "edge_weight": jnp.clip(jnp.exp(math.log(1.0) - 2.3025851 * jax.random.uniform(splits[11], (NB, NODES), jnp.float32) ** levels(splits[11], (NB, NODES), ((1, 16),), -0.2, 0.2)), 0.1, 1.0),
        "node_shift": jnp.clip(jnp.exp(math.log(12.0) - 1.3862944 * jax.random.uniform(splits[12], (NODES,), jnp.float32) ** levels(splits[12], (NODES,), ((0, 16),), -0.2, 0.2)), 3.0, 12.0),
        "send_rows": touch_ends(jax.random.randint(splits[13], (SUBS, 2, BORDER), 0, OWN), jax.random.fold_in(splits[13], 1), 0, OWN - 1).astype(jnp.int32),
    }


FLOOR_SHARE = 0.3
EPSILON = 1e-06

def pick_rows(block_rows, chosen):
    return block_rows[chosen]

def extend(vector, send_rows):
    blocks = vector.reshape(SUBS, OWN, SRC)
    picked = jax.vmap(pick_rows)(blocks, send_rows)
    from_lower = jnp.roll(picked[:, 1], 1, axis=0)
    from_upper = jnp.roll(picked[:, 0], -1, axis=0)
    return jnp.concatenate([blocks, from_lower, from_upper], axis=1)

def operate(vector, send_rows, neighbours, edge_weight, node_shift):
    extended = extend(vector, send_rows)
    padded = jnp.concatenate([extended, jnp.zeros((SUBS, 1, SRC), jnp.float32)], axis=1)
    link_table = neighbours.reshape(NB, SUBS, OWN).transpose(1, 0, 2)
    weights = edge_weight.reshape(NB, SUBS, OWN).transpose(1, 0, 2)
    shifts = node_shift.reshape(SUBS, OWN)

    def one_block(block_items):
        ext_rows, link_rows, weight_rows, shift_rows = block_items
        present = jnp.where(link_rows < EXT, weight_rows, jnp.float32(0.0))
        coupled = lax.optimization_barrier(jnp.sum(present[:, :, None] * ext_rows[link_rows], axis=0))
        diagonal = shift_rows + lax.optimization_barrier(jnp.sum(present, axis=0))
        return diagonal[:, None] * ext_rows[:OWN] - coupled
    return lax.map(one_block, (padded, link_table, weights, shifts)).reshape(NODES, SRC)

def precondition(vector, send_rows, lower_inverse, upper_inverse):
    extended = extend(vector, send_rows)

    def one_block(block_items):
        ext_rows, lower_block, upper_block = block_items
        rounded = lax.optimization_barrier(ext_rows.astype(jnp.bfloat16)).astype(jnp.float32)
        inner_part = jnp.dot(lower_block.astype(jnp.float32), rounded, precision=lax.Precision.HIGHEST)
        inner_part = lax.optimization_barrier(inner_part.astype(jnp.bfloat16)).astype(jnp.float32)
        return jnp.dot(upper_block[:OWN].astype(jnp.float32), inner_part, precision=lax.Precision.HIGHEST)
    return lax.map(one_block, (extended, lower_inverse, upper_inverse)).reshape(NODES, SRC)

def column_mean(left_side, right_side):
    return lax.optimization_barrier(jnp.sum(left_side * right_side, axis=0)) / NODES

def reference(solution, residual, shadow, direction, old_image, rho_prev, alpha_prev, omega_prev, lower_inverse, upper_inverse, neighbours, edge_weight, node_shift, send_rows):
    rho_now = column_mean(shadow, residual)
    shadow_square = column_mean(shadow, shadow)
    step_beta = rho_now / rho_prev * (alpha_prev / omega_prev)
    new_direction = residual + step_beta * (direction - omega_prev * old_image)
    direction_hat = precondition(new_direction, send_rows, lower_inverse, upper_inverse)
    image_new = operate(direction_hat, send_rows, neighbours, edge_weight, node_shift)
    denominator = column_mean(shadow, image_new)
    image_square = column_mean(image_new, image_new)
    step_alpha = rho_now / jnp.maximum(denominator, FLOOR_SHARE * jnp.sqrt(shadow_square * image_square))
    middle = residual - step_alpha * image_new
    middle_hat = precondition(middle, send_rows, lower_inverse, upper_inverse)
    tested = operate(middle_hat, send_rows, neighbours, edge_weight, node_shift)
    step_omega = column_mean(tested, middle) / (column_mean(tested, tested) + EPSILON)
    new_solution = solution + step_alpha * direction_hat + step_omega * middle_hat
    new_residual = middle - step_omega * tested
    next_rho = column_mean(shadow, new_residual)
    return (new_solution, new_residual, step_alpha, step_omega, next_rho)
```

```python
import jax
import jax.numpy as jnp
from jax import lax
from jax.sharding import PartitionSpec as P

FLOOR_SHARE = 0.3
EPSILON = 1e-06
AXES = ("sub", "panel")


def sub_sum(values):
    count = lax.axis_size("sub")
    copies = jnp.broadcast_to(values[None], (count,) + values.shape)
    return jnp.sum(lax.all_to_all(copies, "sub", 0, 0), axis=0)


def send(values, route):
    subs = lax.axis_size("sub")
    panels = lax.axis_size("panel")
    pairs = []
    for s in range(subs):
        for p in range(panels):
            target = route(s, p)
            if target is not None:
                pairs.append((s * panels + p, (target[0] % subs) * panels + target[1]))
    return lax.ppermute(values, AXES, pairs)


def matmul(left, right):
    return jnp.dot(left, right, preferred_element_type=jnp.float32)


def per_device(
    solution,
    residual,
    shadow,
    direction,
    old_image,
    rho_prev,
    alpha_prev,
    omega_prev,
    lower_inverse,
    upper_inverse,
    neighbours,
    edge_weight,
    node_shift,
    send_rows,
):
    panel = lax.axis_index("panel")
    first = panel == 0
    own, cols = residual.shape
    node_count = own * lax.axis_size("sub")
    lower = lower_inverse[0]
    ext, half = lower.shape
    upper = upper_inverse[0, :own]
    border = send_rows.shape[2]
    tail = own - half

    present = jnp.where(neighbours < ext, edge_weight, 0.0)
    columns = lax.broadcasted_iota(jnp.int32, (1, ext), 1)
    coupling = jnp.zeros((own, ext), jnp.float32)
    for k in range(neighbours.shape[0]):
        coupling += jnp.where(neighbours[k][:, None] == columns, edge_weight[k][:, None], 0.0)
    coupling = coupling.astype(jnp.bfloat16)
    diagonal = (node_shift + jnp.sum(present, axis=0))[:, None]
    rows = lax.broadcasted_iota(jnp.int32, (1, own), 1)
    select = (send_rows[0].reshape(2 * border, 1) == rows).astype(jnp.bfloat16)

    def by_panel(zero, one):
        return jnp.where(first, zero, one)

    def precondition(vector):
        rounded = vector.astype(jnp.bfloat16)
        ghosts = matmul(select, rounded).astype(jnp.bfloat16)
        down, up = ghosts[:border], ghosts[border:]
        lower0 = send(up, lambda s, p: (s + 1, 1) if p == 0 else None)
        lower1 = send(up, lambda s, p: (s + 1, 1) if p == 1 else None)
        upper0 = send(down, lambda s, p: (s - 1, 1) if p == 0 else None)
        upper1 = send(down, lambda s, p: (s - 1, 1) if p == 1 else None)
        other_head = send(rounded[:half], lambda s, p: (s, 0) if p == 1 else None)
        other_tail = send(rounded[half:], lambda s, p: (s, 1) if p == 0 else None)
        left = by_panel(rounded[:half], jnp.concatenate([other_tail, lower0, upper0], axis=0))
        right = by_panel(other_head, jnp.concatenate([rounded[half:], lower1, upper1], axis=0))
        rhs = jnp.concatenate([left, right], axis=1)
        bottom = matmul(lower[half:], rhs)
        passed = send(bottom.astype(jnp.bfloat16), lambda s, p: (s, 1) if p == 0 else None)
        top = matmul(lower[:half], rhs)
        inner = by_panel(top, bottom + passed.astype(jnp.float32)).astype(jnp.bfloat16)
        part = matmul(upper, inner)
        part_bf = part.astype(jnp.bfloat16)
        edge = matmul(select, part_bf).astype(jnp.bfloat16)
        mine = by_panel(edge[:, :cols], edge[:, cols:])
        others = by_panel(edge[:, cols:], edge[:, :cols])
        same_up = send(mine[border:], lambda s, p: (s + 1, p))
        same_down = send(mine[:border], lambda s, p: (s - 1, p))
        cross_up = send(others[border:], lambda s, p: (s + 1, 1 - p))
        cross_down = send(others[:border], lambda s, p: (s - 1, 1 - p))
        swapped = send(by_panel(part_bf[:, cols:], part_bf[:, :cols]), lambda s, p: (s, 1 - p))
        result = by_panel(part[:, :cols], part[:, cols:]) + swapped.astype(jnp.float32)
        from_lower = same_up.astype(jnp.float32) + cross_up.astype(jnp.float32)
        from_upper = same_down.astype(jnp.float32) + cross_down.astype(jnp.float32)
        return result, from_lower, from_upper

    def operate(result, from_lower, from_upper):
        extended = jnp.concatenate([result, from_lower, from_upper], axis=0).astype(jnp.bfloat16)
        return diagonal * result - matmul(coupling, extended)

    def dots(*pairs):
        return sub_sum(jnp.stack([jnp.sum(a * b, axis=0) for a, b in pairs])) / node_count

    opening = dots((shadow, residual), (shadow, shadow))
    rho_now, shadow_square = opening[0], opening[1]
    step_beta = rho_now / rho_prev * (alpha_prev / omega_prev)
    new_direction = residual + step_beta * (direction - omega_prev * old_image)
    hat_parts = precondition(new_direction)
    direction_hat = hat_parts[0]
    image_new = operate(*hat_parts)
    second = dots((shadow, image_new), (image_new, image_new))
    step_alpha = rho_now / jnp.maximum(second[0], FLOOR_SHARE * jnp.sqrt(shadow_square * second[1]))
    middle = residual - step_alpha * image_new
    hat_parts = precondition(middle)
    middle_hat = hat_parts[0]
    tested = operate(*hat_parts)
    closing = dots((tested, middle), (tested, tested), (shadow, middle), (shadow, tested))
    step_omega = closing[0] / (closing[1] + EPSILON)
    next_rho = closing[2] - step_omega * closing[3]
    new_residual = middle - step_omega * tested
    new_solution = solution + step_alpha * direction_hat + step_omega * middle_hat
    return (new_solution, new_residual, step_alpha, step_omega, next_rho)


def solution(mesh):
    assert mesh.shape["panel"] == 2
    placed = (
        P("sub", "panel"),
        P("sub", "panel"),
        P("sub", "panel"),
        P("sub", "panel"),
        P("sub", "panel"),
        P("panel"),
        P("panel"),
        P("panel"),
        P("sub", None, "panel"),
        P("sub", None, "panel"),
        P(None, "sub"),
        P(None, "sub"),
        P("sub"),
        P("sub", None, None),
    )
    return jax.shard_map(
        per_device,
        mesh=mesh,
        in_specs=placed,
        out_specs=(P("sub", "panel"), P("sub", "panel"), P("panel"), P("panel"), P("panel")),
        check_vma=False,
    )
```

```python
import jax
import jax.numpy as jnp
from jax import lax
from jax.experimental import pallas as pl
from jax.experimental.pallas import tpu as pltpu
from jax.sharding import PartitionSpec as P

FLOOR_SHARE = 0.3
EPSILON = 1e-06
AXES = ("sub", "panel")


def sub_sum(values):
    count = lax.axis_size("sub")
    copies = jnp.broadcast_to(values[None], (count,) + values.shape)
    return jnp.sum(lax.all_to_all(copies, "sub", 0, 0), axis=0)


def send(values, route):
    subs = lax.axis_size("sub")
    panels = lax.axis_size("panel")
    pairs = []
    for s in range(subs):
        for p in range(panels):
            target = route(s, p)
            if target is not None:
                pairs.append((s * panels + p, (target[0] % subs) * panels + target[1]))
    return lax.ppermute(values, AXES, pairs)


def coupling_kernel(neighbours_ref, weight_ref, *refs):
    out_ref, link_rows, weight_rows = refs[-3:]
    link_rows[...] = neighbours_ref[...].T
    weight_rows[...] = weight_ref[...].T
    group = 16
    shape = (group, out_ref.shape[1])
    columns = lax.broadcasted_iota(jnp.int32, shape, 1)

    def body(index, carry):
        rows = pl.ds(index * group, group)
        links, weights = link_rows[rows, :], weight_rows[rows, :]
        total = jnp.zeros(shape, jnp.float32)
        for k in range(links.shape[1]):
            total += jnp.where(links[:, k : k + 1] == columns, weights[:, k : k + 1], 0.0)
        out_ref[rows, :] = total.astype(out_ref.dtype)
        return carry

    lax.fori_loop(0, out_ref.shape[0] // group, body, 0)


def coupling_rows(neighbours, edge_weight, ext, begin, count, before):
    slots, own = neighbours.shape
    rows = 128
    operands = [neighbours, edge_weight]
    in_specs = [pl.BlockSpec((slots, rows), lambda i: (0, i + begin))] * 2
    aliases = {}
    if before is not None:
        operands.append(before)
        in_specs.append(pl.BlockSpec(memory_space=pl.ANY))
        aliases = {2: 0}
    return pl.pallas_call(
        coupling_kernel,
        grid=(count,),
        in_specs=in_specs,
        out_specs=pl.BlockSpec((rows, ext), lambda i: (i + begin, 0)),
        out_shape=jax.ShapeDtypeStruct((own, ext), jnp.bfloat16),
        scratch_shapes=[
            pltpu.VMEM((rows, slots), jnp.int32),
            pltpu.VMEM((rows, slots), jnp.float32),
        ],
        input_output_aliases=aliases,
        cost_estimate=pl.CostEstimate(
            flops=100 * slots * rows * count * ext,
            bytes_accessed=2 * rows * count * ext,
            transcendentals=0,
        ),
    )(*operands)


def matmul(left, right):
    return jnp.dot(left, right, preferred_element_type=jnp.float32)


def per_device(
    solution,
    residual,
    shadow,
    direction,
    old_image,
    rho_prev,
    alpha_prev,
    omega_prev,
    lower_inverse,
    upper_inverse,
    neighbours,
    edge_weight,
    node_shift,
    send_rows,
):
    panel = lax.axis_index("panel")
    first = panel == 0
    own, cols = residual.shape
    node_count = own * lax.axis_size("sub")
    lower = lower_inverse[0]
    ext, half = lower.shape
    upper = upper_inverse[0, :own]
    border = send_rows.shape[2]
    tail = own - half

    blocks = own // 128
    cuts = (0, blocks // 4, blocks // 2, blocks)
    pieces = []

    def next_coupling(trigger):
        at = len(pieces)
        before = pieces[-1] if pieces else None
        trigger, links = lax.optimization_barrier((trigger, neighbours))
        pieces.append(
            coupling_rows(links, edge_weight, ext, cuts[at], cuts[at + 1] - cuts[at], before)
        )
        return trigger

    def meet(arrived):
        arrived, pieces[-1] = lax.optimization_barrier((arrived, pieces[-1]))
        return arrived

    present = jnp.where(neighbours < ext, edge_weight, 0.0)
    diagonal = (node_shift + jnp.sum(present, axis=0))[:, None]
    rows = lax.broadcasted_iota(jnp.int32, (1, own), 1)
    select = (send_rows[0].reshape(2 * border, 1) == rows).astype(jnp.bfloat16)

    def by_panel(zero, one):
        return jnp.where(first, zero, one)

    def precondition(vector, build):
        rounded = vector.astype(jnp.bfloat16)
        ghosts = matmul(select, rounded).astype(jnp.bfloat16)
        head, rest = rounded[:half], jnp.concatenate([rounded[half:], ghosts], axis=0)
        mine, payload = by_panel(head, rest), by_panel(rest, head)
        if build:
            payload = next_coupling(payload)
        received = send(payload, lambda s, p: (s, 1 - p))
        if build:
            received = meet(received)
        pair = by_panel(
            jnp.concatenate([mine, received], axis=1), jnp.concatenate([received, mine], axis=1)
        )
        from_lower = send(pair[tail + border :], lambda s, p: (s + 1, 1) if p == 1 else None)
        from_upper = send(pair[tail : tail + border], lambda s, p: (s - 1, 1) if p == 1 else None)
        bottom = matmul(lower[half:], pair).astype(jnp.bfloat16)
        if build:
            bottom = next_coupling(bottom)
        passed = send(bottom, lambda s, p: (s, 1) if p == 0 else None)
        if build:
            passed = meet(passed)
        rhs = by_panel(pair, jnp.concatenate([pair[:tail], from_lower, from_upper], axis=0))
        diagonal_rows = lax.dynamic_slice_in_dim(lower, panel * half, half, axis=0)
        inner = (matmul(diagonal_rows, rhs) + passed.astype(jnp.float32)).astype(jnp.bfloat16)
        part = matmul(upper, inner)
        part_bf = part.astype(jnp.bfloat16)
        edge = matmul(select, part_bf).astype(jnp.bfloat16)
        mine = by_panel(edge[:, :cols], edge[:, cols:])
        others = by_panel(edge[:, cols:], edge[:, :cols])
        same_up = send(mine[border:], lambda s, p: (s + 1, p))
        same_down = send(mine[:border], lambda s, p: (s - 1, p))
        cross_up = send(others[border:], lambda s, p: (s + 1, 1 - p))
        cross_down = send(others[:border], lambda s, p: (s - 1, 1 - p))
        swapped = send(by_panel(part_bf[:, cols:], part_bf[:, :cols]), lambda s, p: (s, 1 - p))
        result = by_panel(part[:, :cols], part[:, cols:]) + swapped.astype(jnp.float32)
        from_lower = same_up.astype(jnp.float32) + cross_up.astype(jnp.float32)
        from_upper = same_down.astype(jnp.float32) + cross_down.astype(jnp.float32)
        return result, from_lower, from_upper

    def operate(result, from_lower, from_upper):
        extended = jnp.concatenate([result, from_lower, from_upper], axis=0).astype(jnp.bfloat16)
        return diagonal * result - matmul(pieces[-1], extended)

    def partial_dots(*pairs):
        return jnp.stack([jnp.sum(a * b, axis=0) for a, b in pairs])

    def dots(*pairs):
        return sub_sum(partial_dots(*pairs)) / node_count

    sums = next_coupling(partial_dots((shadow, residual), (shadow, shadow)))
    opening = meet(sub_sum(sums)) / node_count
    rho_now, shadow_square = opening[0], opening[1]
    step_beta = rho_now / rho_prev * (alpha_prev / omega_prev)
    new_direction = residual + step_beta * (direction - omega_prev * old_image)
    hat_parts = precondition(new_direction, True)
    direction_hat = hat_parts[0]
    image_new = operate(*hat_parts)
    second = dots((shadow, image_new), (image_new, image_new))
    step_alpha = rho_now / jnp.maximum(second[0], FLOOR_SHARE * jnp.sqrt(shadow_square * second[1]))
    middle = residual - step_alpha * image_new
    hat_parts = precondition(middle, False)
    middle_hat = hat_parts[0]
    tested = operate(*hat_parts)
    closing = dots((tested, middle), (tested, tested), (shadow, middle), (shadow, tested))
    step_omega = closing[0] / (closing[1] + EPSILON)
    next_rho = closing[2] - step_omega * closing[3]
    new_residual = middle - step_omega * tested
    new_solution = solution + step_alpha * direction_hat + step_omega * middle_hat
    return (new_solution, new_residual, step_alpha, step_omega, next_rho)


def solution(mesh):
    assert mesh.shape["panel"] == 2
    placed = (
        P("sub", "panel"),
        P("sub", "panel"),
        P("sub", "panel"),
        P("sub", "panel"),
        P("sub", "panel"),
        P("panel"),
        P("panel"),
        P("panel"),
        P("sub", None, "panel"),
        P("sub", None, "panel"),
        P(None, "sub"),
        P(None, "sub"),
        P("sub"),
        P("sub", None, None),
    )
    return jax.shard_map(
        per_device,
        mesh=mesh,
        in_specs=placed,
        out_specs=(P("sub", "panel"), P("sub", "panel"), P("panel"), P("panel"), P("panel")),
        check_vma=False,
    )
```

```python
import jax
import jax.numpy as jnp
from jax import lax
from jax.experimental import pallas as pl
from jax.experimental.pallas import tpu as pltpu
from jax.sharding import PartitionSpec as P

FLOOR_SHARE = 0.3
EPSILON = 1e-06
AXES = ("sub", "panel")


def sub_sum(values):
    count = lax.axis_size("sub")
    copies = jnp.broadcast_to(values[None], (count,) + values.shape)
    return jnp.sum(lax.all_to_all(copies, "sub", 0, 0), axis=0)


def send(values, route):
    subs = lax.axis_size("sub")
    panels = lax.axis_size("panel")
    pairs = []
    for s in range(subs):
        for p in range(panels):
            target = route(s, p)
            if target is not None:
                pairs.append((s * panels + p, (target[0] % subs) * panels + target[1]))
    return lax.ppermute(values, AXES, pairs)


def merge_repeated(links, weights):
    merged = []
    for k in range(links.shape[0]):
        total = weights[k : k + 1]
        for j in range(k):
            total += jnp.where(links[j : j + 1] == links[k : k + 1], weights[j : j + 1], 0.0)
        merged.append(total)
    return jnp.concatenate(merged, axis=0)


def coupling_kernel(neighbours_ref, weight_ref, *refs):
    out_ref, link_rows, weight_rows = refs[-3:]
    links = neighbours_ref[...]
    link_rows[...] = links.T
    weight_rows[...] = merge_repeated(links, weight_ref[...]).T
    group, lanes = 16, 128
    shape = (group, out_ref.shape[1])
    repeats = shape[1] // lanes
    columns = lax.broadcasted_iota(jnp.int32, shape, 1).astype(jnp.int16)

    def body(index, carry):
        rows = pl.ds(index * group, group)
        links, weights = link_rows[rows, :], weight_rows[rows, :]
        total = jnp.zeros(shape, jnp.bfloat16)
        for k in range(links.shape[1]):
            link = jnp.broadcast_to(links[:, k : k + 1], (group, lanes)).astype(jnp.int16)
            weight = jnp.broadcast_to(weights[:, k : k + 1], (group, lanes)).astype(jnp.bfloat16)
            hit = jnp.concatenate([link] * repeats, axis=1) == columns
            total = jnp.where(hit, jnp.concatenate([weight] * repeats, axis=1), total)
        out_ref[rows, :] = total
        return carry

    lax.fori_loop(0, out_ref.shape[0] // group, body, 0, unroll=4)


def coupling_rows(neighbours, edge_weight, ext, begin, count, before):
    slots, own = neighbours.shape
    rows = 128
    operands = [neighbours, edge_weight]
    in_specs = [pl.BlockSpec((slots, rows), lambda i: (0, i + begin))] * 2
    aliases = {}
    if before is not None:
        operands.append(before)
        in_specs.append(pl.BlockSpec(memory_space=pl.ANY))
        aliases = {2: 0}
    return pl.pallas_call(
        coupling_kernel,
        grid=(count,),
        in_specs=in_specs,
        out_specs=pl.BlockSpec((rows, ext), lambda i: (i + begin, 0)),
        out_shape=jax.ShapeDtypeStruct((own, ext), jnp.bfloat16),
        scratch_shapes=[
            pltpu.VMEM((rows, slots), jnp.int32),
            pltpu.VMEM((rows, slots), jnp.float32),
        ],
        input_output_aliases=aliases,
        cost_estimate=pl.CostEstimate(
            flops=50 * slots * rows * count * ext,
            bytes_accessed=2 * rows * count * ext,
            transcendentals=0,
        ),
    )(*operands)


def matmul(left, right):
    return jnp.dot(left, right, preferred_element_type=jnp.float32)


def per_device(
    solution,
    residual,
    shadow,
    direction,
    old_image,
    rho_prev,
    alpha_prev,
    omega_prev,
    lower_inverse,
    upper_inverse,
    neighbours,
    edge_weight,
    node_shift,
    send_rows,
):
    panel = lax.axis_index("panel")
    first = panel == 0
    own, cols = residual.shape
    node_count = own * lax.axis_size("sub")
    lower = lower_inverse[0]
    ext, half = lower.shape
    upper = upper_inverse[0, :own]
    border = send_rows.shape[2]
    tail = own - half

    blocks = own // 128
    cuts = (0, blocks // 4, blocks // 2, blocks)
    pieces = []

    def next_coupling(trigger):
        at = len(pieces)
        before = pieces[-1] if pieces else None
        trigger, links = lax.optimization_barrier((trigger, neighbours))
        pieces.append(
            coupling_rows(links, edge_weight, ext, cuts[at], cuts[at + 1] - cuts[at], before)
        )
        return trigger

    def meet(arrived):
        arrived, pieces[-1] = lax.optimization_barrier((arrived, pieces[-1]))
        return arrived

    present = jnp.where(neighbours < ext, edge_weight, 0.0)
    diagonal = (node_shift + jnp.sum(present, axis=0))[:, None]
    rows = lax.broadcasted_iota(jnp.int32, (1, own), 1)
    select = (send_rows[0].reshape(2 * border, 1) == rows).astype(jnp.bfloat16)

    def by_panel(zero, one):
        return jnp.where(first, zero, one)

    def precondition(vector, build):
        rounded = vector.astype(jnp.bfloat16)
        ghosts = matmul(select, rounded).astype(jnp.bfloat16)
        head, rest = rounded[:half], jnp.concatenate([rounded[half:], ghosts], axis=0)
        mine, payload = by_panel(head, rest), by_panel(rest, head)
        if build:
            payload = next_coupling(payload)
        received = send(payload, lambda s, p: (s, 1 - p))
        early = matmul(lower[half:], mine).astype(jnp.bfloat16)
        passed_others = send(early, lambda s, p: (s, 1) if p == 0 else None)
        if build:
            received = meet(received)
        pair = jnp.concatenate([received, mine], axis=1)
        from_lower = send(pair[tail + border :], lambda s, p: (s + 1, 1) if p == 1 else None)
        from_upper = send(pair[tail : tail + border], lambda s, p: (s - 1, 1) if p == 1 else None)
        late = matmul(lower[half:], received).astype(jnp.bfloat16)
        if build:
            late = next_coupling(late)
        passed_mine = send(late, lambda s, p: (s, 1) if p == 0 else None)
        if build:
            passed_mine = meet(passed_mine)
        rhs = by_panel(pair, jnp.concatenate([pair[:tail], from_lower, from_upper], axis=0))
        passed = jnp.concatenate([passed_others, passed_mine], axis=1).astype(jnp.float32)
        inner = (matmul(diagonal_rows, rhs) + passed).astype(jnp.bfloat16)
        inner = lax.optimization_barrier(inner)
        part_others = matmul(upper, inner[:, :cols]).astype(jnp.bfloat16)
        part = matmul(upper, inner[:, cols:])
        edge = part[own:].astype(jnp.bfloat16)
        swapped = send(part_others[:own], lambda s, p: (s, 1 - p))
        cross_up = send(part_others[own + border :], lambda s, p: (s + 1, 1 - p))
        cross_down = send(part_others[own : own + border], lambda s, p: (s - 1, 1 - p))
        same_up = send(edge[border:], lambda s, p: (s + 1, p))
        same_down = send(edge[:border], lambda s, p: (s - 1, p))
        result = part[:own] + swapped.astype(jnp.float32)
        from_lower = same_up.astype(jnp.float32) + cross_up.astype(jnp.float32)
        from_upper = same_down.astype(jnp.float32) + cross_down.astype(jnp.float32)
        return result, from_lower, from_upper

    def operate(result, from_lower, from_upper):
        extended = jnp.concatenate([result, from_lower, from_upper], axis=0).astype(jnp.bfloat16)
        return diagonal * result - matmul(pieces[-1], extended)

    def partial_dots(*pairs):
        return jnp.stack([jnp.sum(a * b, axis=0) for a, b in pairs])

    def dots(*pairs):
        return sub_sum(partial_dots(*pairs)) / node_count

    sums = next_coupling(partial_dots((shadow, residual), (shadow, shadow)))
    sums, select, upper = lax.optimization_barrier((sums, select, upper))
    upper = jnp.concatenate([upper, matmul(select, upper).astype(jnp.bfloat16)], axis=0)
    diagonal_rows = lax.dynamic_slice_in_dim(lower, panel * half, half, axis=0)
    opening, upper = lax.optimization_barrier((meet(sub_sum(sums)), upper))
    opening /= node_count
    rho_now, shadow_square = opening[0], opening[1]
    step_beta = rho_now / rho_prev * (alpha_prev / omega_prev)
    new_direction = residual + step_beta * (direction - omega_prev * old_image)
    hat_parts = precondition(new_direction, True)
    direction_hat = hat_parts[0]
    image_new = operate(*hat_parts)
    second = dots((shadow, image_new), (image_new, image_new))
    step_alpha = rho_now / jnp.maximum(second[0], FLOOR_SHARE * jnp.sqrt(shadow_square * second[1]))
    middle = residual - step_alpha * image_new
    hat_parts = precondition(middle, False)
    middle_hat = hat_parts[0]
    tested = operate(*hat_parts)
    closing = dots((tested, middle), (tested, tested), (shadow, middle), (shadow, tested))
    step_omega = closing[0] / (closing[1] + EPSILON)
    next_rho = closing[2] - step_omega * closing[3]
    new_residual = middle - step_omega * tested
    new_solution = solution + step_alpha * direction_hat + step_omega * middle_hat
    return (new_solution, new_residual, step_alpha, step_omega, next_rho)


def solution(mesh):
    assert mesh.shape["panel"] == 2
    placed = (
        P("sub", "panel"),
        P("sub", "panel"),
        P("sub", "panel"),
        P("sub", "panel"),
        P("sub", "panel"),
        P("panel"),
        P("panel"),
        P("panel"),
        P("sub", None, "panel"),
        P("sub", None, "panel"),
        P(None, "sub"),
        P(None, "sub"),
        P("sub"),
        P("sub", None, None),
    )
    return jax.shard_map(
        per_device,
        mesh=mesh,
        in_specs=placed,
        out_specs=(P("sub", "panel"), P("sub", "panel"), P("panel"), P("panel"), P("panel")),
        check_vma=False,
    )
```

```python
import jax
import jax.numpy as jnp
from jax import lax
from jax.experimental import pallas as pl
from jax.experimental.pallas import tpu as pltpu
from jax.sharding import PartitionSpec as P

FLOOR_SHARE = 0.3
EPSILON = 1e-06
AXES = ("sub", "panel")


def send(values, route):
    subs = lax.axis_size("sub")
    panels = lax.axis_size("panel")
    pairs = []
    for s in range(subs):
        for p in range(panels):
            target = route(s, p)
            if target is not None:
                pairs.append((s * panels + p, (target[0] % subs) * panels + target[1]))
    return lax.ppermute(values, AXES, pairs)


def merge_repeated(links, weights):
    merged = []
    for k in range(links.shape[0]):
        total = weights[k : k + 1]
        for j in range(k):
            total += jnp.where(links[j : j + 1] == links[k : k + 1], weights[j : j + 1], 0.0)
        merged.append(total)
    return jnp.concatenate(merged, axis=0)


def coupling_kernel(neighbours_ref, weight_ref, out_ref, link_rows, weight_rows):
    links = neighbours_ref[...]
    link_rows[...] = links.T
    weight_rows[...] = merge_repeated(links, weight_ref[...]).T
    group, lanes = 16, 128
    shape = (group, out_ref.shape[1])
    repeats = shape[1] // lanes
    columns = lax.broadcasted_iota(jnp.int32, shape, 1).astype(jnp.int16)

    def body(index, carry):
        rows = pl.ds(index * group, group)
        links, weights = link_rows[rows, :], weight_rows[rows, :]
        total = jnp.zeros(shape, jnp.bfloat16)
        for k in range(links.shape[1]):
            link = jnp.broadcast_to(links[:, k : k + 1], (group, lanes)).astype(jnp.int16)
            weight = jnp.broadcast_to(weights[:, k : k + 1], (group, lanes)).astype(jnp.bfloat16)
            hit = jnp.concatenate([link] * repeats, axis=1) == columns
            total = jnp.where(hit, jnp.concatenate([weight] * repeats, axis=1), total)
        out_ref[rows, :] = total
        return carry

    lax.fori_loop(0, out_ref.shape[0] // group, body, 0, unroll=4)


def coupling_rows(neighbours, edge_weight, ext, begin, count):
    slots = neighbours.shape[0]
    rows = 128
    return pl.pallas_call(
        coupling_kernel,
        grid=(count,),
        in_specs=[pl.BlockSpec((slots, rows), lambda i: (0, i + begin))] * 2,
        out_specs=pl.BlockSpec((rows, ext), lambda i: (i, 0)),
        out_shape=jax.ShapeDtypeStruct((rows * count, ext), jnp.bfloat16),
        scratch_shapes=[
            pltpu.VMEM((rows, slots), jnp.int32),
            pltpu.VMEM((rows, slots), jnp.float32),
        ],
        cost_estimate=pl.CostEstimate(
            flops=50 * slots * rows * count * ext,
            bytes_accessed=2 * rows * count * ext,
            transcendentals=0,
        ),
        compiler_params=pltpu.CompilerParams(vmem_limit_bytes=8 << 20),
    )(neighbours, edge_weight)


def operate_kernel(closing, *refs):
    part, swapped, same_up, cross_up, same_down, cross_down, diagonal, shadow = refs[:8]
    refs = refs[8:]
    if closing:
        middle, refs = refs[0], refs[1:]
    *weights, hat_ref, image_ref, sums_ref, extended = refs
    own, border = part.shape[0], same_up.shape[0]
    hat = part[...] + swapped[...].astype(jnp.float32)
    hat_ref[...] = hat
    extended[:own] = hat.astype(jnp.bfloat16)
    for at, (same, cross) in enumerate(((same_up, cross_up), (same_down, cross_down))):
        ghost = same[...].astype(jnp.float32) + cross[...].astype(jnp.float32)
        extended[own + at * border : own + (at + 1) * border] = ghost.astype(jnp.bfloat16)
    begin = 0
    sums = 0.0
    for weight in weights:
        rows = slice(begin, begin + weight.shape[0])
        begin += weight.shape[0]
        coupled = jnp.dot(weight[...], extended[...], preferred_element_type=jnp.float32)
        image = diagonal[rows] * hat_ref[rows] - coupled
        image_ref[rows] = image
        if closing:
            pairs = (
                (image, middle[rows]),
                (image, image),
                (shadow[rows], middle[rows]),
                (shadow[rows], image),
            )
        else:
            pairs = ((shadow[rows], image), (image, image))
        sums += jnp.concatenate([jnp.sum(a * b, axis=0, keepdims=True) for a, b in pairs], axis=0)
    sums_ref[...] = jnp.broadcast_to(sums[None], sums_ref.shape)


def operate(parts, diagonal, shadow, middle, coupling, copies):
    closing = middle is not None
    operands = [*parts, diagonal, shadow] + ([middle] if closing else []) + list(coupling)
    own, cols = shadow.shape
    vector = jax.ShapeDtypeStruct((own, cols), jnp.float32)
    count = 4 if closing else 2
    ext = coupling[0].shape[1]
    in_vmem = pl.BlockSpec(memory_space=pltpu.VMEM)
    return pl.pallas_call(
        lambda *refs: operate_kernel(closing, *refs),
        in_specs=[in_vmem] * len(operands),
        out_specs=[in_vmem] * 3,
        out_shape=[vector, vector, jax.ShapeDtypeStruct((copies, count, cols), jnp.float32)],
        scratch_shapes=[pltpu.VMEM((ext, cols), jnp.bfloat16)],
        cost_estimate=pl.CostEstimate(
            flops=2 * own * ext * cols, bytes_accessed=2 * own * ext, transcendentals=0
        ),
        compiler_params=pltpu.CompilerParams(vmem_limit_bytes=24 << 20),
        name="operate_closing" if closing else "operate_second",
    )(*operands)


def matmul(left, right):
    return jnp.dot(left, right, preferred_element_type=jnp.float32)


def per_device(
    solution,
    residual,
    shadow,
    direction,
    old_image,
    rho_prev,
    alpha_prev,
    omega_prev,
    lower_inverse,
    upper_inverse,
    neighbours,
    edge_weight,
    node_shift,
    send_rows,
):
    panel = lax.axis_index("panel")
    first = panel == 0
    own, cols = residual.shape
    node_count = own * lax.axis_size("sub")
    lower = lower_inverse[0]
    ext, half = lower.shape
    upper = upper_inverse[0, :own]
    border = send_rows.shape[2]
    tail = own - half

    blocks = own // 128
    cuts = (0, blocks // 2, blocks)
    coupling = []

    def next_coupling(trigger):
        begin, end = cuts[len(coupling) : len(coupling) + 2]
        trigger, links = lax.optimization_barrier((trigger, neighbours))
        coupling.append(coupling_rows(links, edge_weight, ext, begin, end - begin))
        return trigger

    def meet(arrived, value):
        return lax.optimization_barrier((arrived, value))

    present = jnp.where(neighbours < ext, edge_weight, 0.0)
    diagonal = jnp.broadcast_to((node_shift + jnp.sum(present, axis=0))[:, None], (own, cols))
    rows = lax.broadcasted_iota(jnp.int32, (1, own), 1)
    select = (send_rows[0].reshape(2 * border, 1) == rows).astype(jnp.bfloat16)

    def by_panel(zero, one):
        return jnp.where(first, zero, one)

    diagonal_rows = lax.dynamic_slice_in_dim(lower, panel * half, half, axis=0)

    def precondition(vector, chosen_upper):
        rounded = vector.astype(jnp.bfloat16)
        ghosts = matmul(select, rounded).astype(jnp.bfloat16)
        head, rest = rounded[:half], jnp.concatenate([rounded[half:], ghosts], axis=0)
        mine, payload = by_panel(head, rest), by_panel(rest, head)
        build = chosen_upper is None
        if build:
            payload, chosen = lax.optimization_barrier((payload, select))
            chosen_upper = matmul(chosen, upper).astype(jnp.bfloat16)
        received = send(payload, lambda s, p: (s, 1 - p))
        early = matmul(lower[half:], mine).astype(jnp.bfloat16)
        passed_others = send(early, lambda s, p: (s, 1) if p == 0 else None)
        if build:
            received, chosen_upper = meet(received, chosen_upper)
        pair = jnp.concatenate([received, mine], axis=1)
        up, down = pair[tail + border :], pair[tail : tail + border]
        from_lower = send(up, lambda s, p: (s + 1, 1) if p == 1 else None)
        from_upper = send(down, lambda s, p: (s - 1, 1) if p == 1 else None)
        late = matmul(lower[half:], received).astype(jnp.bfloat16)
        if build:
            late = next_coupling(late)
        passed_mine = send(late, lambda s, p: (s, 1) if p == 0 else None)
        if build:
            passed_mine, coupling[-1] = meet(passed_mine, coupling[-1])
        rhs = by_panel(pair, jnp.concatenate([pair[:tail], from_lower, from_upper], axis=0))
        passed = jnp.concatenate([passed_others, passed_mine], axis=1).astype(jnp.float32)
        inner = (matmul(diagonal_rows, rhs) + passed).astype(jnp.bfloat16)
        inner = lax.optimization_barrier(inner)
        others, mine = inner[:, :cols], inner[:, cols:]
        other_part = matmul(upper, others).astype(jnp.bfloat16)
        other_edge = matmul(chosen_upper, others).astype(jnp.bfloat16)
        swapped = send(other_part, lambda s, p: (s, 1 - p))
        cross_up = send(other_edge[border:], lambda s, p: (s + 1, 1 - p))
        cross_down = send(other_edge[:border], lambda s, p: (s - 1, 1 - p))
        edge = matmul(chosen_upper, mine).astype(jnp.bfloat16)
        part = matmul(upper, mine)
        same_up = send(edge[border:], lambda s, p: (s + 1, p))
        same_down = send(edge[:border], lambda s, p: (s - 1, p))
        return (part, swapped, same_up, cross_up, same_down, cross_down), chosen_upper

    copies = lax.axis_size("sub")

    def sub_mean(values):
        return jnp.sum(lax.all_to_all(values, "sub", 0, 0), axis=0) / node_count

    sums = jnp.stack([jnp.sum(shadow * residual, axis=0), jnp.sum(shadow * shadow, axis=0)])
    sums = next_coupling(jnp.broadcast_to(sums[None], (copies, 2, cols)))
    opening, coupling[-1] = meet(sub_mean(sums), coupling[-1])
    rho_now, shadow_square = opening[0], opening[1]
    step_beta = rho_now / rho_prev * (alpha_prev / omega_prev)
    new_direction = residual + step_beta * (direction - omega_prev * old_image)
    parts, chosen_upper = precondition(new_direction, None)
    direction_hat, image_new, sums = operate(parts, diagonal, shadow, None, coupling, copies)
    second = sub_mean(sums)
    step_alpha = rho_now / jnp.maximum(second[0], FLOOR_SHARE * jnp.sqrt(shadow_square * second[1]))
    middle = residual - step_alpha * image_new
    parts, _ = precondition(middle, chosen_upper)
    middle_hat, tested, sums = operate(parts, diagonal, shadow, middle, coupling, copies)
    closing = sub_mean(sums)
    step_omega = closing[0] / (closing[1] + EPSILON)
    next_rho = closing[2] - step_omega * closing[3]
    new_residual = middle - step_omega * tested
    new_solution = solution + step_alpha * direction_hat + step_omega * middle_hat
    return (new_solution, new_residual, step_alpha, step_omega, next_rho)


def solution(mesh):
    assert mesh.shape["panel"] == 2
    placed = (
        P("sub", "panel"),
        P("sub", "panel"),
        P("sub", "panel"),
        P("sub", "panel"),
        P("sub", "panel"),
        P("panel"),
        P("panel"),
        P("panel"),
        P("sub", None, "panel"),
        P("sub", None, "panel"),
        P(None, "sub"),
        P(None, "sub"),
        P("sub"),
        P("sub", None, None),
    )
    return jax.shard_map(
        per_device,
        mesh=mesh,
        in_specs=placed,
        out_specs=(P("sub", "panel"), P("sub", "panel"), P("panel"), P("panel"), P("panel")),
        check_vma=False,
    )
```

```python
import jax
import jax.numpy as jnp
from jax import lax
from jax.experimental import pallas as pl
from jax.experimental.pallas import tpu as pltpu
from jax.sharding import PartitionSpec as P

FLOOR_SHARE = 0.3
EPSILON = 1e-06
AXES = ("sub", "panel")


def send(values, route):
    subs = lax.axis_size("sub")
    panels = lax.axis_size("panel")
    pairs = []
    for s in range(subs):
        for p in range(panels):
            target = route(s, p)
            if target is not None:
                pairs.append((s * panels + p, (target[0] % subs) * panels + target[1]))
    return lax.ppermute(values, AXES, pairs)


def merge_repeated(links, weights):
    merged = []
    for k in range(links.shape[0]):
        total = weights[k : k + 1]
        for j in range(k):
            total += jnp.where(links[j : j + 1] == links[k : k + 1], weights[j : j + 1], 0.0)
        merged.append(total)
    return jnp.concatenate(merged, axis=0)


def coupling_kernel(neighbours_ref, weight_ref, out_ref, link_rows, weight_rows):
    links = neighbours_ref[...]
    link_rows[...] = links.T
    weight_rows[...] = merge_repeated(links, weight_ref[...]).T
    group, lanes = 16, 128
    shape = (group, out_ref.shape[1])
    repeats = shape[1] // lanes
    columns = lax.broadcasted_iota(jnp.int32, shape, 1).astype(jnp.int16)

    def body(index, carry):
        rows = pl.ds(index * group, group)
        links, weights = link_rows[rows, :], weight_rows[rows, :]
        total = jnp.zeros(shape, jnp.bfloat16)
        for k in range(links.shape[1]):
            link = jnp.broadcast_to(links[:, k : k + 1], (group, lanes)).astype(jnp.int16)
            weight = jnp.broadcast_to(weights[:, k : k + 1], (group, lanes)).astype(jnp.bfloat16)
            hit = jnp.concatenate([link] * repeats, axis=1) == columns
            total = jnp.where(hit, jnp.concatenate([weight] * repeats, axis=1), total)
        out_ref[rows, :] = total
        return carry

    lax.fori_loop(0, out_ref.shape[0] // group, body, 0, unroll=4)


def coupling_rows(neighbours, edge_weight, ext, begin, count):
    slots = neighbours.shape[0]
    rows = 128
    return pl.pallas_call(
        coupling_kernel,
        grid=(count,),
        in_specs=[pl.BlockSpec((slots, rows), lambda i: (0, i + begin))] * 2,
        out_specs=pl.BlockSpec((rows, ext), lambda i: (i, 0)),
        out_shape=jax.ShapeDtypeStruct((rows * count, ext), jnp.bfloat16),
        scratch_shapes=[
            pltpu.VMEM((rows, slots), jnp.int32),
            pltpu.VMEM((rows, slots), jnp.float32),
        ],
        cost_estimate=pl.CostEstimate(
            flops=50 * slots * rows * count * ext,
            bytes_accessed=2 * rows * count * ext,
            transcendentals=0,
        ),
        compiler_params=pltpu.CompilerParams(vmem_limit_bytes=8 << 20),
    )(neighbours, edge_weight)


def operate_kernel(closing, *refs):
    part, swapped, same_near, cross_near, same_far, cross_far, diagonal, shadow = refs[:8]
    refs = refs[8:]
    if closing:
        middle, refs = refs[0], refs[1:]
    *weights, hat_ref, image_ref, sums_ref, extended = refs
    own, border = part.shape[0], same_near.shape[0]
    hat = part[...] + swapped[...].astype(jnp.float32)
    hat_ref[...] = hat
    extended[:own] = hat.astype(jnp.bfloat16)
    for at, (same, cross) in enumerate(((same_near, cross_near), (same_far, cross_far))):
        ghost = same[...].astype(jnp.float32) + cross[...].astype(jnp.float32)
        extended[own + at * border : own + (at + 1) * border] = ghost.astype(jnp.bfloat16)
    begin = 0
    sums = 0.0
    for weight in weights:
        rows = slice(begin, begin + weight.shape[0])
        begin += weight.shape[0]
        coupled = jnp.dot(weight[...], extended[...], preferred_element_type=jnp.float32)
        image = diagonal[rows] * hat_ref[rows] - coupled
        image_ref[rows] = image
        if closing:
            pairs = (
                (image, middle[rows]),
                (image, image),
                (shadow[rows], middle[rows]),
                (shadow[rows], image),
            )
        else:
            pairs = ((shadow[rows], image), (image, image))
        sums += jnp.concatenate([jnp.sum(a * b, axis=0, keepdims=True) for a, b in pairs], axis=0)
    sums_ref[...] = jnp.broadcast_to(sums[None], sums_ref.shape)


def operate(parts, diagonal, shadow, middle, coupling, copies):
    closing = middle is not None
    operands = [*parts, diagonal, shadow] + ([middle] if closing else []) + list(coupling)
    own, cols = shadow.shape
    vector = jax.ShapeDtypeStruct((own, cols), jnp.float32)
    count = 4 if closing else 2
    ext = coupling[0].shape[1]
    in_vmem = pl.BlockSpec(memory_space=pltpu.VMEM)
    return pl.pallas_call(
        lambda *refs: operate_kernel(closing, *refs),
        in_specs=[in_vmem] * len(operands),
        out_specs=[in_vmem] * 3,
        out_shape=[vector, vector, jax.ShapeDtypeStruct((copies, count, cols), jnp.float32)],
        scratch_shapes=[pltpu.VMEM((ext, cols), jnp.bfloat16)],
        cost_estimate=pl.CostEstimate(
            flops=2 * own * ext * cols, bytes_accessed=2 * own * ext, transcendentals=0
        ),
        compiler_params=pltpu.CompilerParams(vmem_limit_bytes=24 << 20),
        name="operate_closing" if closing else "operate_second",
    )(*operands)


def near(s):
    return s ^ 1


def far(s):
    return s - 1 if s % 2 == 0 else s + 1


def matmul(left, right):
    return jnp.dot(left, right, preferred_element_type=jnp.float32)


def per_device(
    solution,
    residual,
    shadow,
    direction,
    old_image,
    rho_prev,
    alpha_prev,
    omega_prev,
    lower_inverse,
    upper_inverse,
    neighbours,
    edge_weight,
    node_shift,
    send_rows,
):
    panel = lax.axis_index("panel")
    first = panel == 0
    own, cols = residual.shape
    node_count = own * lax.axis_size("sub")
    lower = lower_inverse[0]
    ext, half = lower.shape
    upper = upper_inverse[0, :own]
    border = send_rows.shape[2]
    tail = own - half

    blocks = own // 128
    cuts = (0, blocks // 2, blocks)
    coupling = []

    def next_coupling(trigger):
        begin, end = cuts[len(coupling) : len(coupling) + 2]
        trigger, links = lax.optimization_barrier((trigger, neighbours))
        coupling.append(coupling_rows(links, edge_weight, ext, begin, end - begin))
        return trigger

    def meet(arrived, value):
        return lax.optimization_barrier((arrived, value))

    even = lax.axis_index("sub") % 2 == 0

    def by_parity(zero, one):
        return jnp.where(even, zero, one)

    present = jnp.where(neighbours < ext, edge_weight, 0.0)
    turned = jnp.where(neighbours < own + border, neighbours + border, neighbours - border)
    ghost = even & (neighbours >= own) & (neighbours < ext)
    neighbours = jnp.where(ghost, turned, neighbours)
    near_far = by_parity(send_rows[0, ::-1], send_rows[0])
    diagonal = jnp.broadcast_to((node_shift + jnp.sum(present, axis=0))[:, None], (own, cols))
    rows = lax.broadcasted_iota(jnp.int32, (1, own), 1)
    select = (near_far.reshape(2 * border, 1) == rows).astype(jnp.bfloat16)

    def by_panel(zero, one):
        return jnp.where(first, zero, one)

    diagonal_rows = lax.dynamic_slice_in_dim(lower, panel * half, half, axis=0)

    def precondition(vector, chosen_upper):
        rounded = vector.astype(jnp.bfloat16)
        ghosts = matmul(select, rounded).astype(jnp.bfloat16)
        head, rest = rounded[:half], jnp.concatenate([rounded[half:], ghosts], axis=0)
        mine, payload = by_panel(head, rest), by_panel(rest, head)
        build = chosen_upper is None
        received = send(payload, lambda s, p: (s, 1 - p))
        early = matmul(lower[half:], mine).astype(jnp.bfloat16)
        passed_others = send(early, lambda s, p: (s, 1) if p == 0 else None)
        pair = jnp.concatenate([received, mine], axis=1)
        late = matmul(lower[half:], received).astype(jnp.bfloat16)
        if build:
            late, chosen = lax.optimization_barrier((next_coupling(late), select))
            chosen_upper = matmul(chosen, upper).astype(jnp.bfloat16)
        passed_mine = send(late, lambda s, p: (s, 1) if p == 0 else None)
        from_far = send(pair[tail + border :], lambda s, p: (far(s), 1) if p == 1 else None)
        from_near = send(pair[tail : tail + border], lambda s, p: (near(s), 1) if p == 1 else None)
        if build:
            passed_mine, coupling[-1] = meet(passed_mine, coupling[-1])
            passed_mine, chosen_upper = meet(passed_mine, chosen_upper)
        from_lower, from_upper = by_parity(from_far, from_near), by_parity(from_near, from_far)
        rhs = by_panel(pair, jnp.concatenate([pair[:tail], from_lower, from_upper], axis=0))
        passed = jnp.concatenate([passed_others, passed_mine], axis=1).astype(jnp.float32)
        inner = (matmul(diagonal_rows, rhs) + passed).astype(jnp.bfloat16)
        inner = lax.optimization_barrier(inner)
        others, mine = inner[:, :cols], inner[:, cols:]
        other_part = matmul(upper, others).astype(jnp.bfloat16)
        other_edge = matmul(chosen_upper, others).astype(jnp.bfloat16)
        swapped = send(other_part, lambda s, p: (s, 1 - p))
        cross_far = send(other_edge[border:], lambda s, p: (far(s), 1 - p))
        edge = matmul(chosen_upper, mine).astype(jnp.bfloat16)
        part = matmul(upper, mine)
        same_far = send(edge[border:], lambda s, p: (far(s), p))
        cross_near = send(other_edge[:border], lambda s, p: (near(s), 1 - p))
        same_near = send(edge[:border], lambda s, p: (near(s), p))
        return (part, swapped, same_near, cross_near, same_far, cross_far), chosen_upper

    copies = lax.axis_size("sub")

    def sub_mean(values):
        return jnp.sum(lax.all_to_all(values, "sub", 0, 0), axis=0) / node_count

    sums = jnp.stack([jnp.sum(shadow * residual, axis=0), jnp.sum(shadow * shadow, axis=0)])
    sums = next_coupling(jnp.broadcast_to(sums[None], (copies, 2, cols)))
    opening, coupling[-1] = meet(sub_mean(sums), coupling[-1])
    rho_now, shadow_square = opening[0], opening[1]
    step_beta = rho_now / rho_prev * (alpha_prev / omega_prev)
    new_direction = residual + step_beta * (direction - omega_prev * old_image)
    parts, chosen_upper = precondition(new_direction, None)
    direction_hat, image_new, sums = operate(parts, diagonal, shadow, None, coupling, copies)
    second = sub_mean(sums)
    step_alpha = rho_now / jnp.maximum(second[0], FLOOR_SHARE * jnp.sqrt(shadow_square * second[1]))
    middle = residual - step_alpha * image_new
    parts, _ = precondition(middle, chosen_upper)
    middle_hat, tested, sums = operate(parts, diagonal, shadow, middle, coupling, copies)
    closing = sub_mean(sums)
    step_omega = closing[0] / (closing[1] + EPSILON)
    next_rho = closing[2] - step_omega * closing[3]
    new_residual = middle - step_omega * tested
    new_solution = solution + step_alpha * direction_hat + step_omega * middle_hat
    return (new_solution, new_residual, step_alpha, step_omega, next_rho)


def solution(mesh):
    assert mesh.shape["panel"] == 2 and mesh.shape["sub"] % 2 == 0
    placed = (
        P("sub", "panel"),
        P("sub", "panel"),
        P("sub", "panel"),
        P("sub", "panel"),
        P("sub", "panel"),
        P("panel"),
        P("panel"),
        P("panel"),
        P("sub", None, "panel"),
        P("sub", None, "panel"),
        P(None, "sub"),
        P(None, "sub"),
        P("sub"),
        P("sub", None, None),
    )
    return jax.shard_map(
        per_device,
        mesh=mesh,
        in_specs=placed,
        out_specs=(P("sub", "panel"), P("sub", "panel"), P("panel"), P("panel"), P("panel")),
        check_vma=False,
    )
```

```python
import jax
import jax.numpy as jnp
from jax import lax
from jax.experimental import pallas as pl
from jax.experimental.pallas import tpu as pltpu
from jax.sharding import PartitionSpec as P

FLOOR_SHARE = 0.3
EPSILON = 1e-06
AXES = ("sub", "panel")


def send(values, route):
    subs = lax.axis_size("sub")
    panels = lax.axis_size("panel")
    pairs = []
    for s in range(subs):
        for p in range(panels):
            target = route(s, p)
            if target is not None:
                pairs.append((s * panels + p, (target[0] % subs) * panels + target[1]))
    return lax.ppermute(values, AXES, pairs)


def merge_repeated(links, weights):
    merged = []
    for k in range(links.shape[0]):
        total = weights[k : k + 1]
        for j in range(k):
            total += jnp.where(links[j : j + 1] == links[k : k + 1], weights[j : j + 1], 0.0)
        merged.append(total)
    return jnp.concatenate(merged, axis=0)


def coupling_kernel(neighbours_ref, weight_ref, out_ref, link_rows, weight_rows):
    links = neighbours_ref[...]
    link_rows[...] = links.T
    weight_rows[...] = merge_repeated(links, weight_ref[...]).T
    group, lanes = 16, 128
    shape = (group, out_ref.shape[1])
    repeats = shape[1] // lanes
    columns = lax.broadcasted_iota(jnp.int32, shape, 1).astype(jnp.int16)

    def body(index, carry):
        rows = pl.ds(index * group, group)
        links, weights = link_rows[rows, :], weight_rows[rows, :]
        total = jnp.zeros(shape, jnp.bfloat16)
        for k in range(links.shape[1]):
            link = jnp.broadcast_to(links[:, k : k + 1], (group, lanes)).astype(jnp.int16)
            weight = jnp.broadcast_to(weights[:, k : k + 1], (group, lanes)).astype(jnp.bfloat16)
            hit = jnp.concatenate([link] * repeats, axis=1) == columns
            total = jnp.where(hit, jnp.concatenate([weight] * repeats, axis=1), total)
        out_ref[rows, :] = total
        return carry

    lax.fori_loop(0, out_ref.shape[0] // group, body, 0, unroll=4)


def coupling_rows(neighbours, edge_weight, ext, begin, count):
    slots = neighbours.shape[0]
    rows = 128
    return pl.pallas_call(
        coupling_kernel,
        grid=(count,),
        in_specs=[pl.BlockSpec((slots, rows), lambda i: (0, i + begin))] * 2,
        out_specs=pl.BlockSpec((rows, ext), lambda i: (i, 0)),
        out_shape=jax.ShapeDtypeStruct((rows * count, ext), jnp.bfloat16),
        scratch_shapes=[
            pltpu.VMEM((rows, slots), jnp.int32),
            pltpu.VMEM((rows, slots), jnp.float32),
        ],
        cost_estimate=pl.CostEstimate(
            flops=50 * slots * rows * count * ext,
            bytes_accessed=2 * rows * count * ext,
            transcendentals=0,
        ),
        compiler_params=pltpu.CompilerParams(vmem_limit_bytes=8 << 20),
    )(neighbours, edge_weight)


def operate_kernel(closing, *refs):
    part, swapped, same_near, cross_near, same_far, cross_far, diagonal, shadow = refs[:8]
    refs = refs[8:]
    if closing:
        middle, refs = refs[0], refs[1:]
    *weights, hat_out, image_out, sums_ref, extended, hat_ref, image_ref, done = refs
    own, border = part.shape[0], same_near.shape[0]
    hat = part[...] + swapped[...].astype(jnp.float32)
    hat_ref[...] = hat
    extended[:own] = hat.astype(jnp.bfloat16)
    for at, (same, cross) in enumerate(((same_near, cross_near), (same_far, cross_far))):
        ghost = same[...].astype(jnp.float32) + cross[...].astype(jnp.float32)
        extended[own + at * border : own + (at + 1) * border] = ghost.astype(jnp.bfloat16)
    begin = 0
    sums = 0.0
    leaving = [pltpu.make_async_copy(hat_ref, hat_out, done.at[0])]
    leaving[0].start()
    for weight in weights:
        rows = slice(begin, begin + weight.shape[0])
        begin += weight.shape[0]
        coupled = jnp.dot(weight[...], extended[...], preferred_element_type=jnp.float32)
        image = diagonal[rows] * hat_ref[rows] - coupled
        image_ref[rows] = image
        leaving.append(
            pltpu.make_async_copy(image_ref.at[rows], image_out.at[rows], done.at[len(leaving)])
        )
        leaving[-1].start()
        if closing:
            pairs = (
                (image, middle[rows]),
                (image, image),
                (shadow[rows], middle[rows]),
                (shadow[rows], image),
            )
        else:
            pairs = ((shadow[rows], image), (image, image))
        sums += jnp.concatenate([jnp.sum(a * b, axis=0, keepdims=True) for a, b in pairs], axis=0)
    sums_ref[...] = jnp.broadcast_to(sums[None], sums_ref.shape)
    for copy in leaving:
        copy.wait()


def operate(parts, diagonal, shadow, middle, coupling, copies):
    closing = middle is not None
    operands = [*parts, diagonal, shadow] + ([middle] if closing else []) + list(coupling)
    own, cols = shadow.shape
    vector = jax.ShapeDtypeStruct((own, cols), jnp.float32)
    count = 4 if closing else 2
    ext = coupling[0].shape[1]
    in_vmem = pl.BlockSpec(memory_space=pltpu.VMEM)
    return pl.pallas_call(
        lambda *refs: operate_kernel(closing, *refs),
        in_specs=[in_vmem] * len(operands),
        out_specs=[pl.BlockSpec(memory_space=pltpu.HBM)] * 2 + [in_vmem],
        out_shape=[vector, vector, jax.ShapeDtypeStruct((copies, count, cols), jnp.float32)],
        scratch_shapes=[
            pltpu.VMEM((ext, cols), jnp.bfloat16),
            pltpu.VMEM((own, cols), jnp.float32),
            pltpu.VMEM((own, cols), jnp.float32),
            pltpu.SemaphoreType.DMA((1 + len(coupling),)),
        ],
        cost_estimate=pl.CostEstimate(
            flops=2 * own * ext * cols, bytes_accessed=2 * own * ext, transcendentals=0
        ),
        compiler_params=pltpu.CompilerParams(vmem_limit_bytes=24 << 20),
        name="operate_closing" if closing else "operate_second",
    )(*operands)


def split_rows(vector, select, panel, mine_ref, payload_ref):
    rounded = vector.astype(jnp.bfloat16)
    half = mine_ref.shape[0]
    tail = rounded.shape[0] - half
    ghosts = jnp.dot(select[...], rounded, preferred_element_type=jnp.float32)
    ghosts = ghosts.astype(jnp.bfloat16)

    def put(head_ref, rest_ref):
        head_ref[...] = rounded[:half]
        rest_ref[:tail] = rounded[half:]
        rest_ref[tail:] = ghosts

    pl.when(panel[0] == 0)(lambda: put(mine_ref, payload_ref))
    pl.when(panel[0] != 0)(lambda: put(payload_ref, mine_ref))


def direction_kernel(node_count, panel, sums, past, residual, direction, old_image, select, *outs):
    means_ref, mine_ref, payload_ref = outs
    means = jnp.sum(sums[...], axis=0) / node_count
    means_ref[...] = means
    rho_prev, alpha_prev, omega_prev = past[0:1], past[1:2], past[2:3]
    step_beta = means[0:1] / rho_prev * (alpha_prev / omega_prev)
    vector = residual[...] + step_beta * (direction[...] - omega_prev * old_image[...])
    split_rows(vector, select, panel, mine_ref, payload_ref)


def middle_kernel(node_count, panel, sums, opening, residual, image, select, *outs):
    alpha_ref, middle_ref, mine_ref, payload_ref = outs
    means = jnp.sum(sums[...], axis=0) / node_count
    floor = FLOOR_SHARE * jnp.sqrt(opening[1:2] * means[1:2])
    step_alpha = opening[0:1] / jnp.maximum(means[0:1], floor)
    alpha_ref[...] = step_alpha
    middle = residual[...] - step_alpha * image[...]
    middle_ref[...] = middle
    split_rows(middle, select, panel, mine_ref, payload_ref)


def small_call(kernel, panel, operands, outs):
    in_vmem = pl.BlockSpec(memory_space=pltpu.VMEM)
    return pl.pallas_call(
        kernel,
        in_specs=[pl.BlockSpec(memory_space=pltpu.SMEM)] + [in_vmem] * len(operands),
        out_specs=[in_vmem] * len(outs),
        out_shape=outs,
        compiler_params=pltpu.CompilerParams(vmem_limit_bytes=12 << 20),
    )(panel.reshape(1), *operands)


def near(s):
    return s ^ 1


def far(s):
    return s - 1 if s % 2 == 0 else s + 1


def matmul(left, right):
    return jnp.dot(left, right, preferred_element_type=jnp.float32)


def per_device(
    solution,
    residual,
    shadow,
    direction,
    old_image,
    rho_prev,
    alpha_prev,
    omega_prev,
    lower_inverse,
    upper_inverse,
    neighbours,
    edge_weight,
    node_shift,
    send_rows,
):
    panel = lax.axis_index("panel")
    first = panel == 0
    own, cols = residual.shape
    node_count = own * lax.axis_size("sub")
    lower = lower_inverse[0]
    ext, half = lower.shape
    upper = upper_inverse[0, :own]
    border = send_rows.shape[2]
    tail = own - half

    blocks = own // 128
    cuts = (0, blocks // 2, blocks)
    coupling = []

    def next_coupling(trigger):
        begin, end = cuts[len(coupling) : len(coupling) + 2]
        trigger, links = lax.optimization_barrier((trigger, neighbours))
        coupling.append(coupling_rows(links, edge_weight, ext, begin, end - begin))
        return trigger

    def meet(arrived, value):
        return lax.optimization_barrier((arrived, value))

    even = lax.axis_index("sub") % 2 == 0

    def by_parity(zero, one):
        return jnp.where(even, zero, one)

    turned = jnp.where(neighbours < own + border, neighbours + border, neighbours - border)
    ghost = even & (neighbours >= own) & (neighbours < ext)
    neighbours = jnp.where(ghost, turned, neighbours)
    near_far = by_parity(send_rows[0, ::-1], send_rows[0])
    rows = lax.broadcasted_iota(jnp.int32, (1, own), 1)

    def by_panel(zero, one):
        return jnp.where(first, zero, one)

    diagonal_rows = lax.dynamic_slice_in_dim(lower, panel * half, half, axis=0)

    def precondition(mine, payload, chosen_upper):
        build = chosen_upper is None
        if build:
            payload = next_coupling(payload)
        received = send(payload, lambda s, p: (s, 1 - p))
        early = matmul(lower[half:], mine).astype(jnp.bfloat16)
        passed_others = send(early, lambda s, p: (s, 1) if p == 0 else None)
        if build:
            received, coupling[-1] = meet(received, coupling[-1])
        late = matmul(lower[half:], received).astype(jnp.bfloat16)
        if build:
            late, chosen = lax.optimization_barrier((next_coupling(late), select))
            chosen_upper = matmul(chosen, upper).astype(jnp.bfloat16)
        passed_mine = send(late, lambda s, p: (s, 1) if p == 0 else None)
        near_rows, far_rows = slice(tail, tail + border), slice(tail + border, half)

        def both(part):
            return jnp.concatenate([received[part], mine[part]], axis=1)

        from_far = send(both(far_rows), lambda s, p: (far(s), 1) if p == 1 else None)
        from_near = send(both(near_rows), lambda s, p: (near(s), 1) if p == 1 else None)
        if build:
            passed_mine, coupling[-1] = meet(passed_mine, coupling[-1])
            passed_mine, chosen_upper = meet(passed_mine, chosen_upper)
        from_lower, from_upper = by_parity(from_far, from_near), by_parity(from_near, from_far)

        def solve(kept, ghost_columns, passed):
            ghosts = [from_lower[:, ghost_columns], from_upper[:, ghost_columns]]
            rhs = by_panel(kept, jnp.concatenate([kept[:tail], *ghosts], axis=0))
            product = matmul(diagonal_rows, rhs) + passed.astype(jnp.float32)
            return lax.optimization_barrier(product.astype(jnp.bfloat16))

        others = solve(received, slice(0, cols), passed_others)
        if build:
            others, links = lax.optimization_barrier((others, neighbours))
            present = jnp.where(links < ext, edge_weight, 0.0)
            scale = jnp.broadcast_to((node_shift + jnp.sum(present, axis=0))[:, None], (own, cols))
            diagonal.append(scale)
        other_part = matmul(upper, others).astype(jnp.bfloat16)
        swapped = send(other_part, lambda s, p: (s, 1 - p))
        mine = solve(mine, slice(cols, 2 * cols), passed_mine)
        other_edge = matmul(chosen_upper, others).astype(jnp.bfloat16)
        cross_far = send(other_edge[border:], lambda s, p: (far(s), 1 - p))
        edge = matmul(chosen_upper, mine).astype(jnp.bfloat16)
        part = matmul(upper, mine)
        same_far = send(edge[border:], lambda s, p: (far(s), p))
        cross_near = send(other_edge[:border], lambda s, p: (near(s), 1 - p))
        same_near = send(edge[:border], lambda s, p: (near(s), p))
        return (part, swapped, same_near, cross_near, same_far, cross_far), chosen_upper

    copies = lax.axis_size("sub")

    def exchange(values):
        return lax.all_to_all(values, "sub", 0, 0)

    diagonal = []
    vector = jax.ShapeDtypeStruct((own, cols), jnp.float32)
    panel_rows = jax.ShapeDtypeStruct((half, cols), jnp.bfloat16)
    sums = jnp.stack([jnp.sum(shadow * residual, axis=0), jnp.sum(shadow * shadow, axis=0)])
    sums = jnp.broadcast_to(sums[None], (copies, 2, cols))
    sums, near_far = lax.optimization_barrier((sums, near_far))
    select = (near_far.reshape(2 * border, 1) == rows).astype(jnp.bfloat16)
    past = jnp.stack([rho_prev, alpha_prev, omega_prev])
    opening, mine, payload = small_call(
        lambda *refs: direction_kernel(node_count, *refs),
        panel,
        (exchange(sums), past, residual, direction, old_image, select),
        [jax.ShapeDtypeStruct((2, cols), jnp.float32), panel_rows, panel_rows],
    )
    parts, chosen_upper = precondition(mine, payload, None)
    direction_hat, image_new, sums = operate(parts, diagonal[0], shadow, None, coupling, copies)
    step_alpha, middle, mine, payload = small_call(
        lambda *refs: middle_kernel(node_count, *refs),
        panel,
        (exchange(sums), opening, residual, image_new, select),
        [jax.ShapeDtypeStruct((1, cols), jnp.float32), vector, panel_rows, panel_rows],
    )
    step_alpha = step_alpha[0]
    parts, _ = precondition(mine, payload, chosen_upper)
    middle_hat, tested, sums = operate(parts, diagonal[0], shadow, middle, coupling, copies)
    closing = jnp.sum(exchange(sums), axis=0) / node_count
    step_omega = closing[0] / (closing[1] + EPSILON)
    next_rho = closing[2] - step_omega * closing[3]
    new_residual = middle - step_omega * tested
    new_solution = solution + step_alpha * direction_hat + step_omega * middle_hat
    return (new_solution, new_residual, step_alpha, step_omega, next_rho)


def solution(mesh):
    assert mesh.shape["panel"] == 2 and mesh.shape["sub"] % 2 == 0
    placed = (
        P("sub", "panel"),
        P("sub", "panel"),
        P("sub", "panel"),
        P("sub", "panel"),
        P("sub", "panel"),
        P("panel"),
        P("panel"),
        P("panel"),
        P("sub", None, "panel"),
        P("sub", None, "panel"),
        P(None, "sub"),
        P(None, "sub"),
        P("sub"),
        P("sub", None, None),
    )
    return jax.shard_map(
        per_device,
        mesh=mesh,
        in_specs=placed,
        out_specs=(P("sub", "panel"), P("sub", "panel"), P("panel"), P("panel"), P("panel")),
        check_vma=False,
    )
```

```python
import jax
import jax.numpy as jnp
from jax import lax
from jax.experimental import pallas as pl
from jax.experimental.pallas import tpu as pltpu
from jax.sharding import PartitionSpec as P

FLOOR_SHARE = 0.3
EPSILON = 1e-06
AXES = ("sub", "panel")


def send(values, route):
    subs = lax.axis_size("sub")
    panels = lax.axis_size("panel")
    pairs = []
    for s in range(subs):
        for p in range(panels):
            target = route(s, p)
            if target is not None:
                pairs.append((s * panels + p, (target[0] % subs) * panels + target[1]))
    return lax.ppermute(values, AXES, pairs)


def merge_repeated(links, weights):
    merged = []
    for k in range(links.shape[0]):
        total = weights[k : k + 1]
        for j in range(k):
            total += jnp.where(links[j : j + 1] == links[k : k + 1], weights[j : j + 1], 0.0)
        merged.append(total)
    return jnp.concatenate(merged, axis=0)


def coupling_kernel(neighbours_ref, weight_ref, out_ref, link_rows, weight_rows):
    links = neighbours_ref[...]
    link_rows[...] = links.T
    weight_rows[...] = merge_repeated(links, weight_ref[...]).T
    group, lanes = 16, 128
    shape = (group, out_ref.shape[1])
    repeats = shape[1] // lanes
    columns = lax.broadcasted_iota(jnp.int32, shape, 1).astype(jnp.int16)

    def body(index, carry):
        rows = pl.ds(index * group, group)
        links, weights = link_rows[rows, :], weight_rows[rows, :]
        total = jnp.zeros(shape, jnp.bfloat16)
        for k in range(links.shape[1]):
            link = jnp.broadcast_to(links[:, k : k + 1], (group, lanes)).astype(jnp.int16)
            weight = jnp.broadcast_to(weights[:, k : k + 1], (group, lanes)).astype(jnp.bfloat16)
            hit = jnp.concatenate([link] * repeats, axis=1) == columns
            total = jnp.where(hit, jnp.concatenate([weight] * repeats, axis=1), total)
        out_ref[rows, :] = total
        return carry

    lax.fori_loop(0, out_ref.shape[0] // group, body, 0, unroll=4)


def coupling_rows(neighbours, edge_weight, ext, begin, count):
    slots = neighbours.shape[0]
    rows = 128
    return pl.pallas_call(
        coupling_kernel,
        grid=(count,),
        in_specs=[pl.BlockSpec((slots, rows), lambda i: (0, i + begin))] * 2,
        out_specs=pl.BlockSpec((rows, ext), lambda i: (i, 0)),
        out_shape=jax.ShapeDtypeStruct((rows * count, ext), jnp.bfloat16),
        scratch_shapes=[
            pltpu.VMEM((rows, slots), jnp.int32),
            pltpu.VMEM((rows, slots), jnp.float32),
        ],
        cost_estimate=pl.CostEstimate(
            flops=50 * slots * rows * count * ext,
            bytes_accessed=2 * rows * count * ext,
            transcendentals=0,
        ),
        compiler_params=pltpu.CompilerParams(vmem_limit_bytes=8 << 20),
    )(neighbours, edge_weight)


def operate_kernel(closing, *refs):
    part, swapped, same_near, cross_near, same_far, cross_far, diagonal, shadow = refs[:8]
    refs = refs[8:]
    if closing:
        middle, refs = refs[0], refs[1:]
    *weights, hat_out, image_out, sums_ref, extended, hat_ref, image_ref, done = refs
    own, border = part.shape[0], same_near.shape[0]
    hat = part[...] + swapped[...].astype(jnp.float32)
    hat_ref[...] = hat
    extended[:own] = hat.astype(jnp.bfloat16)
    for at, (same, cross) in enumerate(((same_near, cross_near), (same_far, cross_far))):
        ghost = same[...].astype(jnp.float32) + cross[...].astype(jnp.float32)
        extended[own + at * border : own + (at + 1) * border] = ghost.astype(jnp.bfloat16)
    begin = 0
    sums = 0.0
    leaving = [pltpu.make_async_copy(hat_ref, hat_out, done.at[0])]
    leaving[0].start()
    for weight in weights:
        rows = slice(begin, begin + weight.shape[0])
        begin += weight.shape[0]
        coupled = jnp.dot(weight[...], extended[...], preferred_element_type=jnp.float32)
        image = diagonal[rows] * hat_ref[rows] - coupled
        image_ref[rows] = image
        leaving.append(
            pltpu.make_async_copy(image_ref.at[rows], image_out.at[rows], done.at[len(leaving)])
        )
        leaving[-1].start()
        if closing:
            pairs = (
                (image, middle[rows]),
                (image, image),
                (shadow[rows], middle[rows]),
                (shadow[rows], image),
            )
        else:
            pairs = ((shadow[rows], image), (image, image))
        sums += jnp.concatenate([jnp.sum(a * b, axis=0, keepdims=True) for a, b in pairs], axis=0)
    sums_ref[...] = jnp.broadcast_to(sums[None], sums_ref.shape)
    for copy in leaving:
        copy.wait()


def operate(parts, diagonal, shadow, middle, coupling, copies):
    closing = middle is not None
    operands = [*parts, diagonal, shadow] + ([middle] if closing else []) + list(coupling)
    own, cols = shadow.shape
    vector = jax.ShapeDtypeStruct((own, cols), jnp.float32)
    count = 4 if closing else 2
    ext = coupling[0].shape[1]
    in_vmem = pl.BlockSpec(memory_space=pltpu.VMEM)
    return pl.pallas_call(
        lambda *refs: operate_kernel(closing, *refs),
        in_specs=[in_vmem] * len(operands),
        out_specs=[pl.BlockSpec(memory_space=pltpu.HBM)] * 2 + [in_vmem],
        out_shape=[vector, vector, jax.ShapeDtypeStruct((copies, count, cols), jnp.float32)],
        scratch_shapes=[
            pltpu.VMEM((ext, cols), jnp.bfloat16),
            pltpu.VMEM((own, cols), jnp.float32),
            pltpu.VMEM((own, cols), jnp.float32),
            pltpu.SemaphoreType.DMA((1 + len(coupling),)),
        ],
        cost_estimate=pl.CostEstimate(
            flops=2 * own * ext * cols, bytes_accessed=2 * own * ext, transcendentals=0
        ),
        compiler_params=pltpu.CompilerParams(vmem_limit_bytes=24 << 20),
        name="operate_closing" if closing else "operate_second",
    )(*operands)


def round_and_select(vector, select, rounded_ref, ghosts_ref):
    rounded = vector.astype(jnp.bfloat16)
    rounded_ref[...] = rounded
    ghosts = jnp.dot(select[...], rounded, preferred_element_type=jnp.float32)
    ghosts_ref[...] = ghosts.astype(jnp.bfloat16)


def direction_kernel(node_count, sums, past, residual, direction, old_image, select, *outs):
    means_ref, rounded_ref, ghosts_ref = outs
    means = jnp.sum(sums[...], axis=0) / node_count
    means_ref[...] = means
    rho_prev, alpha_prev, omega_prev = past[0:1], past[1:2], past[2:3]
    step_beta = means[0:1] / rho_prev * (alpha_prev / omega_prev)
    vector = residual[...] + step_beta * (direction[...] - omega_prev * old_image[...])
    round_and_select(vector, select, rounded_ref, ghosts_ref)


def middle_kernel(node_count, sums, opening, residual, image, select, *outs):
    alpha_ref, middle_ref, rounded_ref, ghosts_ref = outs
    means = jnp.sum(sums[...], axis=0) / node_count
    floor = FLOOR_SHARE * jnp.sqrt(opening[1:2] * means[1:2])
    step_alpha = opening[0:1] / jnp.maximum(means[0:1], floor)
    alpha_ref[...] = step_alpha
    middle = residual[...] - step_alpha * image[...]
    middle_ref[...] = middle
    round_and_select(middle, select, rounded_ref, ghosts_ref)


def small_call(kernel, operands, outs):
    in_vmem = pl.BlockSpec(memory_space=pltpu.VMEM)
    return pl.pallas_call(
        kernel,
        in_specs=[in_vmem] * len(operands),
        out_specs=[in_vmem] * len(outs),
        out_shape=outs,
        compiler_params=pltpu.CompilerParams(vmem_limit_bytes=12 << 20),
    )(*operands)


def near(s):
    return s ^ 1


def far(s):
    return s - 1 if s % 2 == 0 else s + 1


def matmul(left, right):
    return jnp.dot(left, right, preferred_element_type=jnp.float32)


def per_device(
    solution,
    residual,
    shadow,
    direction,
    old_image,
    rho_prev,
    alpha_prev,
    omega_prev,
    lower_inverse,
    upper_inverse,
    neighbours,
    edge_weight,
    node_shift,
    send_rows,
):
    panel = lax.axis_index("panel")
    first = panel == 0
    own, cols = residual.shape
    node_count = own * lax.axis_size("sub")
    lower = lower_inverse[0]
    ext, half = lower.shape
    upper = upper_inverse[0, :own]
    border = send_rows.shape[2]

    blocks = own // 128
    cuts = (0, blocks // 2, blocks)
    coupling = []

    def next_coupling():
        begin, end = cuts[len(coupling) : len(coupling) + 2]
        coupling.append(coupling_rows(neighbours, edge_weight, ext, begin, end - begin))

    def meet(arrived, value):
        return lax.optimization_barrier((arrived, value))

    even = lax.axis_index("sub") % 2 == 0

    def by_parity(zero, one):
        return jnp.where(even, zero, one)

    turned = jnp.where(neighbours < own + border, neighbours + border, neighbours - border)
    ghost = even & (neighbours >= own) & (neighbours < ext)
    neighbours = jnp.where(ghost, turned, neighbours)
    rows = lax.broadcasted_iota(jnp.int32, (1, own), 1)

    def by_panel(zero, one):
        return jnp.where(first, zero, one)

    diagonal_rows = lax.dynamic_slice_in_dim(lower, panel * half, half, axis=0)

    def precondition(rounded, ghosts, build):
        head, rest = rounded[:half], rounded[half:]
        near_rows, far_rows = ghosts[:border], ghosts[border:]
        early = matmul(lower[half:], head).astype(jnp.bfloat16)
        payload = by_panel(jnp.concatenate([early, rest], axis=0), rounded)
        received = send(payload, lambda s, p: (s, 1 - p))
        far_cross = send(far_rows, lambda s, p: (far(s), 1) if p == 0 else None)
        far_same = send(far_rows, lambda s, p: (far(s), 1) if p == 1 else None)
        near_cross = send(near_rows, lambda s, p: (near(s), 1) if p == 0 else None)
        near_same = send(near_rows, lambda s, p: (near(s), 1) if p == 1 else None)
        if build:
            next_coupling()
            received, coupling[-1] = meet(received, coupling[-1])
        late = matmul(lower[half:], received[:half]).astype(jnp.bfloat16)
        passed_mine = send(late, lambda s, p: (s, 1) if p == 0 else None)

        def solve(kept, last, from_far, from_near, passed):
            lower_upper = [by_parity(from_far, from_near), by_parity(from_near, from_far)]
            rhs = by_panel(kept, jnp.concatenate([last, *lower_upper], axis=0))
            product = matmul(diagonal_rows, rhs) + passed.astype(jnp.float32)
            return lax.optimization_barrier(product.astype(jnp.bfloat16))

        passed_others = by_panel(jnp.zeros_like(head), received[:half])
        others = solve(received[:half], received[half:], far_cross, near_cross, passed_others)
        if build:
            others, links = lax.optimization_barrier((others, neighbours))
            present = jnp.where(links < ext, edge_weight, 0.0)
            scale = jnp.broadcast_to((node_shift + jnp.sum(present, axis=0))[:, None], (own, cols))
            diagonal.append(scale)
        other_part = matmul(upper, others).astype(jnp.bfloat16)
        swapped = send(other_part, lambda s, p: (s, 1 - p))
        other_edge = matmul(chosen_upper, others).astype(jnp.bfloat16)
        cross_far = send(other_edge[border:], lambda s, p: (far(s), 1 - p))
        cross_near = send(other_edge[:border], lambda s, p: (near(s), 1 - p))
        mine = solve(head, rest, far_same, near_same, passed_mine)
        edge = matmul(chosen_upper, mine).astype(jnp.bfloat16)
        part = matmul(upper, mine)
        same_far = send(edge[border:], lambda s, p: (far(s), p))
        same_near = send(edge[:border], lambda s, p: (near(s), p))
        if build:
            next_coupling()
            swapped, coupling[-1] = meet(swapped, coupling[-1])
        return part, swapped, same_near, cross_near, same_far, cross_far

    copies = lax.axis_size("sub")

    def exchange(values):
        return lax.all_to_all(values, "sub", 0, 0)

    diagonal = []
    vector = jax.ShapeDtypeStruct((own, cols), jnp.float32)
    narrow = [jax.ShapeDtypeStruct((count, cols), jnp.bfloat16) for count in (own, 2 * border)]
    sums = jnp.stack([jnp.sum(shadow * residual, axis=0), jnp.sum(shadow * shadow, axis=0)])
    sums = jnp.broadcast_to(sums[None], (copies, 2, cols))
    sums, lists = lax.optimization_barrier((sums, send_rows))
    near_far = [by_parity(lists[0, 1], lists[0, 0]), by_parity(lists[0, 0], lists[0, 1])]
    select = jnp.concatenate(near_far)[:, None] == rows
    select = select.astype(jnp.bfloat16)
    chosen_upper = matmul(select, upper).astype(jnp.bfloat16)
    opening_sums, chosen_upper = meet(exchange(sums), chosen_upper)
    past = jnp.stack([rho_prev, alpha_prev, omega_prev])
    opening, rounded, ghosts = small_call(
        lambda *refs: direction_kernel(node_count, *refs),
        (opening_sums, past, residual, direction, old_image, select),
        [jax.ShapeDtypeStruct((2, cols), jnp.float32), *narrow],
    )
    parts = precondition(rounded, ghosts, True)
    direction_hat, image_new, sums = operate(parts, diagonal[0], shadow, None, coupling, copies)
    step_alpha, middle, rounded, ghosts = small_call(
        lambda *refs: middle_kernel(node_count, *refs),
        (exchange(sums), opening, residual, image_new, select),
        [jax.ShapeDtypeStruct((1, cols), jnp.float32), vector, *narrow],
    )
    step_alpha = step_alpha[0]
    parts = precondition(rounded, ghosts, False)
    middle_hat, tested, sums = operate(parts, diagonal[0], shadow, middle, coupling, copies)
    closing = jnp.sum(exchange(sums), axis=0) / node_count
    step_omega = closing[0] / (closing[1] + EPSILON)
    next_rho = closing[2] - step_omega * closing[3]
    new_residual = middle - step_omega * tested
    new_solution = solution + step_alpha * direction_hat + step_omega * middle_hat
    return (new_solution, new_residual, step_alpha, step_omega, next_rho)


def solution(mesh):
    assert mesh.shape["panel"] == 2 and mesh.shape["sub"] % 2 == 0
    placed = (
        P("sub", "panel"),
        P("sub", "panel"),
        P("sub", "panel"),
        P("sub", "panel"),
        P("sub", "panel"),
        P("panel"),
        P("panel"),
        P("panel"),
        P("sub", None, "panel"),
        P("sub", None, "panel"),
        P(None, "sub"),
        P(None, "sub"),
        P("sub"),
        P("sub", None, None),
    )
    return jax.shard_map(
        per_device,
        mesh=mesh,
        in_specs=placed,
        out_specs=(P("sub", "panel"), P("sub", "panel"), P("panel"), P("panel"), P("panel")),
        check_vma=False,
    )
```

```python
import jax
import jax.numpy as jnp
from jax import lax
from jax.experimental import pallas as pl
from jax.experimental.pallas import tpu as pltpu
from jax.sharding import PartitionSpec as P

FLOOR_SHARE = 0.3
EPSILON = 1e-06
AXES = ("sub", "panel")


def send(values, route):
    subs = lax.axis_size("sub")
    panels = lax.axis_size("panel")
    pairs = []
    for s in range(subs):
        for p in range(panels):
            target = route(s, p)
            if target is not None:
                pairs.append((s * panels + p, (target[0] % subs) * panels + target[1]))
    return lax.ppermute(values, AXES, pairs)


def merge_repeated(links, weights):
    merged = []
    for k in range(links.shape[0]):
        total = weights[k : k + 1]
        for j in range(k):
            total += jnp.where(links[j : j + 1] == links[k : k + 1], weights[j : j + 1], 0.0)
        merged.append(total)
    return jnp.concatenate(merged, axis=0)


def coupling_kernel(neighbours_ref, weight_ref, out_ref, link_rows, weight_rows):
    links = neighbours_ref[...]
    link_rows[...] = links.T
    weight_rows[...] = merge_repeated(links, weight_ref[...]).T
    group, lanes = 16, 128
    shape = (group, out_ref.shape[1])
    repeats = shape[1] // lanes
    columns = lax.broadcasted_iota(jnp.int32, shape, 1).astype(jnp.int16)

    def body(index, carry):
        rows = pl.ds(index * group, group)
        links, weights = link_rows[rows, :], weight_rows[rows, :]
        total = jnp.zeros(shape, jnp.bfloat16)
        for k in range(links.shape[1]):
            link = jnp.broadcast_to(links[:, k : k + 1], (group, lanes)).astype(jnp.int16)
            weight = jnp.broadcast_to(weights[:, k : k + 1], (group, lanes)).astype(jnp.bfloat16)
            hit = jnp.concatenate([link] * repeats, axis=1) == columns
            total = jnp.where(hit, jnp.concatenate([weight] * repeats, axis=1), total)
        out_ref[rows, :] = total
        return carry

    lax.fori_loop(0, out_ref.shape[0] // group, body, 0, unroll=4)


def coupling_rows(neighbours, edge_weight, ext, begin, count):
    slots = neighbours.shape[0]
    rows = 128
    return pl.pallas_call(
        coupling_kernel,
        grid=(count,),
        in_specs=[pl.BlockSpec((slots, rows), lambda i: (0, i + begin))] * 2,
        out_specs=pl.BlockSpec((rows, ext), lambda i: (i, 0)),
        out_shape=jax.ShapeDtypeStruct((rows * count, ext), jnp.bfloat16),
        scratch_shapes=[
            pltpu.VMEM((rows, slots), jnp.int32),
            pltpu.VMEM((rows, slots), jnp.float32),
        ],
        cost_estimate=pl.CostEstimate(
            flops=50 * slots * rows * count * ext,
            bytes_accessed=2 * rows * count * ext,
            transcendentals=0,
        ),
        compiler_params=pltpu.CompilerParams(vmem_limit_bytes=8 << 20),
    )(neighbours, edge_weight)


def operate_kernel(closing, *refs):
    part, swapped, same_near, cross_near, same_far, cross_far, diagonal, shadow = refs[:8]
    refs = refs[8:]
    if closing:
        middle, refs = refs[0], refs[1:]
    *weights, hat_out, image_out, sums_ref, extended, hat_ref, image_ref, done = refs
    own, border = part.shape[0], same_near.shape[0]
    hat = part[...] + swapped[...].astype(jnp.float32)
    hat_ref[...] = hat
    extended[:own] = hat.astype(jnp.bfloat16)
    for at, (same, cross) in enumerate(((same_near, cross_near), (same_far, cross_far))):
        ghost = same[...].astype(jnp.float32) + cross[...].astype(jnp.float32)
        extended[own + at * border : own + (at + 1) * border] = ghost.astype(jnp.bfloat16)
    begin = 0
    sums = 0.0
    leaving = [pltpu.make_async_copy(hat_ref, hat_out, done.at[0])]
    leaving[0].start()
    for weight in weights:
        rows = slice(begin, begin + weight.shape[0])
        begin += weight.shape[0]
        coupled = jnp.dot(weight[...], extended[...], preferred_element_type=jnp.float32)
        image = diagonal[rows] * hat_ref[rows] - coupled
        image_ref[rows] = image
        leaving.append(
            pltpu.make_async_copy(image_ref.at[rows], image_out.at[rows], done.at[len(leaving)])
        )
        leaving[-1].start()
        if closing:
            pairs = (
                (image, middle[rows]),
                (image, image),
                (shadow[rows], middle[rows]),
                (shadow[rows], image),
            )
        else:
            pairs = ((shadow[rows], image), (image, image))
        sums += jnp.concatenate([jnp.sum(a * b, axis=0, keepdims=True) for a, b in pairs], axis=0)
    sums_ref[...] = jnp.broadcast_to(sums[None], sums_ref.shape)
    for copy in leaving:
        copy.wait()


def operate(parts, diagonal, shadow, middle, coupling, copies):
    closing = middle is not None
    operands = [*parts, diagonal, shadow] + ([middle] if closing else []) + list(coupling)
    own, cols = shadow.shape
    vector = jax.ShapeDtypeStruct((own, cols), jnp.float32)
    count = 4 if closing else 2
    ext = coupling[0].shape[1]
    in_vmem = pl.BlockSpec(memory_space=pltpu.VMEM)
    return pl.pallas_call(
        lambda *refs: operate_kernel(closing, *refs),
        in_specs=[in_vmem] * len(operands),
        out_specs=[pl.BlockSpec(memory_space=pltpu.HBM)] * 2 + [in_vmem],
        out_shape=[vector, vector, jax.ShapeDtypeStruct((copies, count, cols), jnp.float32)],
        scratch_shapes=[
            pltpu.VMEM((ext, cols), jnp.bfloat16),
            pltpu.VMEM((own, cols), jnp.float32),
            pltpu.VMEM((own, cols), jnp.float32),
            pltpu.SemaphoreType.DMA((1 + len(coupling),)),
        ],
        cost_estimate=pl.CostEstimate(
            flops=2 * own * ext * cols, bytes_accessed=2 * own * ext, transcendentals=0
        ),
        compiler_params=pltpu.CompilerParams(vmem_limit_bytes=24 << 20),
        name="operate_closing" if closing else "operate_second",
    )(*operands)


def split_rows(vector, select, panel, mine_ref, payload_ref):
    rounded = vector.astype(jnp.bfloat16)
    half = mine_ref.shape[0]
    tail = rounded.shape[0] - half
    ghosts = jnp.dot(select[...], rounded, preferred_element_type=jnp.float32)
    ghosts = ghosts.astype(jnp.bfloat16)

    def put(head_ref, rest_ref):
        head_ref[...] = rounded[:half]
        rest_ref[:tail] = rounded[half:]
        rest_ref[tail:] = ghosts

    pl.when(panel[0] == 0)(lambda: put(mine_ref, payload_ref))
    pl.when(panel[0] != 0)(lambda: put(payload_ref, mine_ref))


def opening_kernel(panel, shadow, residual, sums_ref):
    left = shadow[...]
    pairs = (left * residual[...], left * left)
    sums = jnp.concatenate([jnp.sum(p, axis=0, keepdims=True) for p in pairs], axis=0)
    sums_ref[...] = jnp.broadcast_to(sums[None], sums_ref.shape)


def direction_kernel(node_count, panel, sums, past, residual, direction, old_image, select, *outs):
    means_ref, mine_ref, payload_ref = outs
    means = jnp.sum(sums[...], axis=0) / node_count
    means_ref[...] = means
    rho_prev, alpha_prev, omega_prev = past[0:1], past[1:2], past[2:3]
    step_beta = means[0:1] / rho_prev * (alpha_prev / omega_prev)
    vector = residual[...] + step_beta * (direction[...] - omega_prev * old_image[...])
    split_rows(vector, select, panel, mine_ref, payload_ref)


def middle_kernel(node_count, panel, sums, opening, residual, image, select, *outs):
    alpha_ref, middle_ref, mine_ref, payload_ref = outs
    means = jnp.sum(sums[...], axis=0) / node_count
    floor = FLOOR_SHARE * jnp.sqrt(opening[1:2] * means[1:2])
    step_alpha = opening[0:1] / jnp.maximum(means[0:1], floor)
    alpha_ref[...] = step_alpha
    middle = residual[...] - step_alpha * image[...]
    middle_ref[...] = middle
    split_rows(middle, select, panel, mine_ref, payload_ref)


def small_call(kernel, panel, operands, outs):
    in_vmem = pl.BlockSpec(memory_space=pltpu.VMEM)
    return pl.pallas_call(
        kernel,
        in_specs=[pl.BlockSpec(memory_space=pltpu.SMEM)] + [in_vmem] * len(operands),
        out_specs=[in_vmem] * len(outs),
        out_shape=outs,
        compiler_params=pltpu.CompilerParams(vmem_limit_bytes=12 << 20),
    )(panel.reshape(1), *operands)


def near(s):
    return s ^ 1


def far(s):
    return s - 1 if s % 2 == 0 else s + 1


def matmul(left, right):
    return jnp.dot(left, right, preferred_element_type=jnp.float32)


def per_device(
    solution,
    residual,
    shadow,
    direction,
    old_image,
    rho_prev,
    alpha_prev,
    omega_prev,
    lower_inverse,
    upper_inverse,
    neighbours,
    edge_weight,
    node_shift,
    send_rows,
):
    panel = lax.axis_index("panel")
    first = panel == 0
    own, cols = residual.shape
    node_count = own * lax.axis_size("sub")
    lower = lower_inverse[0]
    ext, half = lower.shape
    upper = upper_inverse[0, :own]
    border = send_rows.shape[2]
    tail = own - half

    blocks = own // 128
    cuts = (0, blocks // 4, 5 * blocks // 8, blocks)
    coupling = []

    def next_coupling():
        begin, end = cuts[len(coupling) : len(coupling) + 2]
        coupling.append(coupling_rows(links, edge_weight, ext, begin, end - begin))

    def meet(arrived, value):
        return lax.optimization_barrier((arrived, value))

    even = lax.axis_index("sub") % 2 == 0

    def by_parity(zero, one):
        return jnp.where(even, zero, one)

    rows = lax.broadcasted_iota(jnp.int32, (1, own), 1)

    def by_panel(zero, one):
        return jnp.where(first, zero, one)

    diagonal_rows = lax.dynamic_slice_in_dim(lower, panel * half, half, axis=0)

    def precondition(mine, payload, chosen_upper):
        build = chosen_upper is None
        received = send(payload, lambda s, p: (s, 1 - p))
        early = matmul(lower[half:], mine).astype(jnp.bfloat16)
        passed_others = send(early, lambda s, p: (s, 1) if p == 0 else None)
        if build:
            next_coupling()
            received, coupling[-1] = meet(received, coupling[-1])
        near_rows, far_rows = slice(tail, tail + border), slice(tail + border, half)

        def both(part):
            return jnp.concatenate([received[part], mine[part]], axis=1)

        from_far = send(both(far_rows), lambda s, p: (far(s), 1) if p == 1 else None)
        from_near = send(both(near_rows), lambda s, p: (near(s), 1) if p == 1 else None)
        late = matmul(lower[half:], received).astype(jnp.bfloat16)
        if build:
            late, chosen = lax.optimization_barrier((late, select))
            chosen_upper = matmul(chosen, upper).astype(jnp.bfloat16)
        passed_mine = send(late, lambda s, p: (s, 1) if p == 0 else None)
        if build:
            from_far, chosen_upper = meet(from_far, chosen_upper)
        from_lower, from_upper = by_parity(from_far, from_near), by_parity(from_near, from_far)

        def solve(kept, ghost_columns, passed):
            ghosts = [from_lower[:, ghost_columns], from_upper[:, ghost_columns]]
            rhs = by_panel(kept, jnp.concatenate([kept[:tail], *ghosts], axis=0))
            product = matmul(diagonal_rows, rhs) + passed.astype(jnp.float32)
            return lax.optimization_barrier(product.astype(jnp.bfloat16))

        others = solve(received, slice(0, cols), passed_others)
        if build:
            others, listed = lax.optimization_barrier((others, neighbours))
            present = jnp.where(listed < ext, edge_weight, 0.0)
            scale = jnp.broadcast_to((node_shift + jnp.sum(present, axis=0))[:, None], (own, cols))
            diagonal.append(scale)
        other_part = matmul(upper, others).astype(jnp.bfloat16)
        swapped = send(other_part, lambda s, p: (s, 1 - p))
        other_edge = matmul(chosen_upper, others).astype(jnp.bfloat16)
        cross_far = send(other_edge[border:], lambda s, p: (far(s), 1 - p))
        cross_near = send(other_edge[:border], lambda s, p: (near(s), 1 - p))
        mine = solve(mine, slice(cols, 2 * cols), passed_mine)
        edge = matmul(chosen_upper, mine).astype(jnp.bfloat16)
        part = matmul(upper, mine)
        same_far = send(edge[border:], lambda s, p: (far(s), p))
        same_near = send(edge[:border], lambda s, p: (near(s), p))
        if build:
            next_coupling()
            swapped, coupling[-1] = meet(swapped, coupling[-1])
        return (part, swapped, same_near, cross_near, same_far, cross_far), chosen_upper

    copies = lax.axis_size("sub")

    def exchange(values):
        return lax.all_to_all(values, "sub", 0, 0)

    diagonal = []
    vector = jax.ShapeDtypeStruct((own, cols), jnp.float32)
    panel_rows = jax.ShapeDtypeStruct((half, cols), jnp.bfloat16)
    (sums,) = small_call(
        opening_kernel,
        panel,
        (shadow, residual),
        [jax.ShapeDtypeStruct((copies, 2, cols), jnp.float32)],
    )
    sums, lists, links = lax.optimization_barrier((sums, send_rows, neighbours))
    turned = jnp.where(links < own + border, links + border, links - border)
    ghost = even & (links >= own) & (links < ext)
    links = jnp.where(ghost, turned, links)
    next_coupling()
    opening_sums, coupling[-1] = meet(exchange(sums), coupling[-1])
    near_far = [by_parity(lists[0, 1], lists[0, 0]), by_parity(lists[0, 0], lists[0, 1])]
    select = (jnp.concatenate(near_far)[:, None] == rows).astype(jnp.bfloat16)
    past = jnp.stack([rho_prev, alpha_prev, omega_prev])
    opening, mine, payload = small_call(
        lambda *refs: direction_kernel(node_count, *refs),
        panel,
        (opening_sums, past, residual, direction, old_image, select),
        [jax.ShapeDtypeStruct((2, cols), jnp.float32), panel_rows, panel_rows],
    )
    parts, chosen_upper = precondition(mine, payload, None)
    direction_hat, image_new, sums = operate(parts, diagonal[0], shadow, None, coupling, copies)
    step_alpha, middle, mine, payload = small_call(
        lambda *refs: middle_kernel(node_count, *refs),
        panel,
        (exchange(sums), opening, residual, image_new, select),
        [jax.ShapeDtypeStruct((1, cols), jnp.float32), vector, panel_rows, panel_rows],
    )
    step_alpha = step_alpha[0]
    parts, _ = precondition(mine, payload, chosen_upper)
    middle_hat, tested, sums = operate(parts, diagonal[0], shadow, middle, coupling, copies)
    closing = jnp.sum(exchange(sums), axis=0) / node_count
    step_omega = closing[0] / (closing[1] + EPSILON)
    next_rho = closing[2] - step_omega * closing[3]
    new_residual = middle - step_omega * tested
    new_solution = solution + step_alpha * direction_hat + step_omega * middle_hat
    return (new_solution, new_residual, step_alpha, step_omega, next_rho)


def solution(mesh):
    assert mesh.shape["panel"] == 2 and mesh.shape["sub"] % 2 == 0
    placed = (
        P("sub", "panel"),
        P("sub", "panel"),
        P("sub", "panel"),
        P("sub", "panel"),
        P("sub", "panel"),
        P("panel"),
        P("panel"),
        P("panel"),
        P("sub", None, "panel"),
        P("sub", None, "panel"),
        P(None, "sub"),
        P(None, "sub"),
        P("sub"),
        P("sub", None, None),
    )
    return jax.shard_map(
        per_device,
        mesh=mesh,
        in_specs=placed,
        out_specs=(P("sub", "panel"), P("sub", "panel"), P("panel"), P("panel"), P("panel")),
        check_vma=False,
    )
```

```python
import jax
import jax.numpy as jnp
from jax import lax
from jax.experimental import pallas as pl
from jax.experimental.pallas import tpu as pltpu
from jax.sharding import PartitionSpec as P

FLOOR_SHARE = 0.3
EPSILON = 1e-06
AXES = ("sub", "panel")


def send(values, route):
    subs = lax.axis_size("sub")
    panels = lax.axis_size("panel")
    pairs = []
    for s in range(subs):
        for p in range(panels):
            target = route(s, p)
            if target is not None:
                pairs.append((s * panels + p, (target[0] % subs) * panels + target[1]))
    return lax.ppermute(values, AXES, pairs)


def merge_repeated(links, weights):
    merged = []
    for k in range(links.shape[0]):
        total = weights[k : k + 1]
        for j in range(k):
            total += jnp.where(links[j : j + 1] == links[k : k + 1], weights[j : j + 1], 0.0)
        merged.append(total)
    return jnp.concatenate(merged, axis=0)


def coupling_kernel(neighbours_ref, weight_ref, out_ref, link_rows, weight_rows):
    links = neighbours_ref[...]
    link_rows[...] = links.T
    weight_rows[...] = merge_repeated(links, weight_ref[...]).T
    group, lanes = 16, 128
    shape = (group, out_ref.shape[1])
    repeats = shape[1] // lanes
    columns = lax.broadcasted_iota(jnp.int32, shape, 1).astype(jnp.int16)

    def body(index, carry):
        rows = pl.ds(index * group, group)
        links, weights = link_rows[rows, :], weight_rows[rows, :]
        total = jnp.zeros(shape, jnp.bfloat16)
        for k in range(links.shape[1]):
            link = jnp.broadcast_to(links[:, k : k + 1], (group, lanes)).astype(jnp.int16)
            weight = jnp.broadcast_to(weights[:, k : k + 1], (group, lanes)).astype(jnp.bfloat16)
            hit = jnp.concatenate([link] * repeats, axis=1) == columns
            total = jnp.where(hit, jnp.concatenate([weight] * repeats, axis=1), total)
        out_ref[rows, :] = total
        return carry

    lax.fori_loop(0, out_ref.shape[0] // group, body, 0, unroll=4)


def coupling_rows(neighbours, edge_weight, ext, begin, count):
    slots = neighbours.shape[0]
    rows = 128
    return pl.pallas_call(
        coupling_kernel,
        grid=(count,),
        in_specs=[pl.BlockSpec((slots, rows), lambda i: (0, i + begin))] * 2,
        out_specs=pl.BlockSpec((rows, ext), lambda i: (i, 0)),
        out_shape=jax.ShapeDtypeStruct((rows * count, ext), jnp.bfloat16),
        scratch_shapes=[
            pltpu.VMEM((rows, slots), jnp.int32),
            pltpu.VMEM((rows, slots), jnp.float32),
        ],
        cost_estimate=pl.CostEstimate(
            flops=50 * slots * rows * count * ext,
            bytes_accessed=2 * rows * count * ext,
            transcendentals=0,
        ),
        compiler_params=pltpu.CompilerParams(vmem_limit_bytes=8 << 20),
    )(neighbours, edge_weight)


def operate_kernel(closing, *refs):
    part, swapped, same_near, cross_near, same_far, cross_far, diagonal, shadow = refs[:8]
    refs = refs[8:]
    if closing:
        middle, refs = refs[0], refs[1:]
    *weights, hat_out, image_out, sums_ref, extended, hat_ref, image_ref, done = refs
    own, border = part.shape[0], same_near.shape[0]
    hat = part[...] + swapped[...].astype(jnp.float32)
    hat_ref[...] = hat
    extended[:own] = hat.astype(jnp.bfloat16)
    for at, (same, cross) in enumerate(((same_near, cross_near), (same_far, cross_far))):
        ghost = same[...].astype(jnp.float32) + cross[...].astype(jnp.float32)
        extended[own + at * border : own + (at + 1) * border] = ghost.astype(jnp.bfloat16)
    begin = 0
    sums = 0.0
    leaving = [pltpu.make_async_copy(hat_ref, hat_out, done.at[0])]
    leaving[0].start()
    for weight in weights:
        rows = slice(begin, begin + weight.shape[0])
        begin += weight.shape[0]
        coupled = jnp.dot(weight[...], extended[...], preferred_element_type=jnp.float32)
        image = diagonal[rows] * hat_ref[rows] - coupled
        image_ref[rows] = image
        leaving.append(
            pltpu.make_async_copy(image_ref.at[rows], image_out.at[rows], done.at[len(leaving)])
        )
        leaving[-1].start()
        if closing:
            pairs = (
                (image, middle[rows]),
                (image, image),
                (shadow[rows], middle[rows]),
                (shadow[rows], image),
            )
        else:
            pairs = ((shadow[rows], image), (image, image))
        sums += jnp.concatenate([jnp.sum(a * b, axis=0, keepdims=True) for a, b in pairs], axis=0)
    sums_ref[...] = jnp.broadcast_to(sums[None], sums_ref.shape)
    for copy in leaving:
        copy.wait()


def operate(parts, diagonal, shadow, middle, coupling, copies):
    closing = middle is not None
    operands = [*parts, diagonal, shadow] + ([middle] if closing else []) + list(coupling)
    own, cols = shadow.shape
    vector = jax.ShapeDtypeStruct((own, cols), jnp.float32)
    count = 4 if closing else 2
    ext = coupling[0].shape[1]
    in_vmem = pl.BlockSpec(memory_space=pltpu.VMEM)
    return pl.pallas_call(
        lambda *refs: operate_kernel(closing, *refs),
        in_specs=[in_vmem] * len(operands),
        out_specs=[pl.BlockSpec(memory_space=pltpu.HBM)] * 2 + [in_vmem],
        out_shape=[vector, vector, jax.ShapeDtypeStruct((copies, count, cols), jnp.float32)],
        scratch_shapes=[
            pltpu.VMEM((ext, cols), jnp.bfloat16),
            pltpu.VMEM((own, cols), jnp.float32),
            pltpu.VMEM((own, cols), jnp.float32),
            pltpu.SemaphoreType.DMA((1 + len(coupling),)),
        ],
        cost_estimate=pl.CostEstimate(
            flops=2 * own * ext * cols, bytes_accessed=2 * own * ext, transcendentals=0
        ),
        compiler_params=pltpu.CompilerParams(vmem_limit_bytes=24 << 20),
        name="operate_closing" if closing else "operate_second",
    )(*operands)


def split_rows(vector, select, panel, mine_ref, payload_ref):
    rounded = vector.astype(jnp.bfloat16)
    half = mine_ref.shape[0]
    tail = rounded.shape[0] - half
    ghosts = jnp.dot(select[...], rounded, preferred_element_type=jnp.float32)
    ghosts = ghosts.astype(jnp.bfloat16)

    def put(head_ref, rest_ref):
        head_ref[...] = rounded[:half]
        rest_ref[:tail] = rounded[half:]
        rest_ref[tail:] = ghosts

    pl.when(panel[0] == 0)(lambda: put(mine_ref, payload_ref))
    pl.when(panel[0] != 0)(lambda: put(payload_ref, mine_ref))


def direction_kernel(node_count, panel, sums, past, residual, direction, old_image, select, *outs):
    means_ref, mine_ref, payload_ref = outs
    means = jnp.sum(sums[...], axis=0) / node_count
    means_ref[...] = means
    rho_prev, alpha_prev, omega_prev = past[0:1], past[1:2], past[2:3]
    step_beta = means[0:1] / rho_prev * (alpha_prev / omega_prev)
    vector = residual[...] + step_beta * (direction[...] - omega_prev * old_image[...])
    split_rows(vector, select, panel, mine_ref, payload_ref)


def middle_kernel(node_count, panel, sums, opening, residual, image, select, *outs):
    alpha_ref, middle_ref, mine_ref, payload_ref = outs
    means = jnp.sum(sums[...], axis=0) / node_count
    floor = FLOOR_SHARE * jnp.sqrt(opening[1:2] * means[1:2])
    step_alpha = opening[0:1] / jnp.maximum(means[0:1], floor)
    alpha_ref[...] = step_alpha
    middle = residual[...] - step_alpha * image[...]
    middle_ref[...] = middle
    split_rows(middle, select, panel, mine_ref, payload_ref)


def small_call(kernel, panel, operands, outs):
    in_vmem = pl.BlockSpec(memory_space=pltpu.VMEM)
    return pl.pallas_call(
        kernel,
        in_specs=[pl.BlockSpec(memory_space=pltpu.SMEM)] + [in_vmem] * len(operands),
        out_specs=[in_vmem] * len(outs),
        out_shape=outs,
        compiler_params=pltpu.CompilerParams(vmem_limit_bytes=12 << 20),
    )(panel.reshape(1), *operands)


def near(s):
    return s ^ 1


def far(s):
    return s - 1 if s % 2 == 0 else s + 1


def matmul(left, right):
    return jnp.dot(left, right, preferred_element_type=jnp.float32)


def per_device(
    solution,
    residual,
    shadow,
    direction,
    old_image,
    rho_prev,
    alpha_prev,
    omega_prev,
    lower_inverse,
    upper_inverse,
    neighbours,
    edge_weight,
    node_shift,
    send_rows,
):
    panel = lax.axis_index("panel")
    first = panel == 0
    own, cols = residual.shape
    node_count = own * lax.axis_size("sub")
    lower = lower_inverse[0]
    ext, half = lower.shape
    upper = upper_inverse[0, :own]
    border = send_rows.shape[2]
    tail = own - half

    blocks = own // 128
    cuts = (0, blocks // 2, blocks)
    coupling = []

    def next_coupling():
        begin, end = cuts[len(coupling) : len(coupling) + 2]
        coupling.append(coupling_rows(neighbours, edge_weight, ext, begin, end - begin))

    def meet(arrived, value):
        return lax.optimization_barrier((arrived, value))

    even = lax.axis_index("sub") % 2 == 0

    def by_parity(zero, one):
        return jnp.where(even, zero, one)

    turned = jnp.where(neighbours < own + border, neighbours + border, neighbours - border)
    ghost = even & (neighbours >= own) & (neighbours < ext)
    neighbours = jnp.where(ghost, turned, neighbours)
    rows = lax.broadcasted_iota(jnp.int32, (1, own), 1)

    def by_panel(zero, one):
        return jnp.where(first, zero, one)

    diagonal_rows = lax.dynamic_slice_in_dim(lower, panel * half, half, axis=0)

    def precondition(mine, payload, build):
        received = send(payload, lambda s, p: (s, 1 - p))
        early = matmul(lower[half:], mine).astype(jnp.bfloat16)
        passed_others = send(early, lambda s, p: (s, 1) if p == 0 else None)
        if build:
            next_coupling()
            received, coupling[-1] = meet(received, coupling[-1])
        near_rows, far_rows = slice(tail, tail + border), slice(tail + border, half)

        def both(part):
            return jnp.concatenate([received[part], mine[part]], axis=1)

        from_far = send(both(far_rows), lambda s, p: (far(s), 1) if p == 1 else None)
        from_near = send(both(near_rows), lambda s, p: (near(s), 1) if p == 1 else None)
        late = matmul(lower[half:], received).astype(jnp.bfloat16)
        passed_mine = send(late, lambda s, p: (s, 1) if p == 0 else None)
        from_lower, from_upper = by_parity(from_far, from_near), by_parity(from_near, from_far)

        def solve(kept, ghost_columns, passed):
            ghosts = [from_lower[:, ghost_columns], from_upper[:, ghost_columns]]
            rhs = by_panel(kept, jnp.concatenate([kept[:tail], *ghosts], axis=0))
            product = matmul(diagonal_rows, rhs) + passed.astype(jnp.float32)
            return lax.optimization_barrier(product.astype(jnp.bfloat16))

        others = solve(received, slice(0, cols), passed_others)
        if build:
            others, links = lax.optimization_barrier((others, neighbours))
            present = jnp.where(links < ext, edge_weight, 0.0)
            scale = jnp.broadcast_to((node_shift + jnp.sum(present, axis=0))[:, None], (own, cols))
            diagonal.append(scale)
        other_part = matmul(upper, others).astype(jnp.bfloat16)
        swapped = send(other_part, lambda s, p: (s, 1 - p))
        other_edge = matmul(chosen_upper, others).astype(jnp.bfloat16)
        cross_far = send(other_edge[border:], lambda s, p: (far(s), 1 - p))
        cross_near = send(other_edge[:border], lambda s, p: (near(s), 1 - p))
        mine = solve(mine, slice(cols, 2 * cols), passed_mine)
        edge = matmul(chosen_upper, mine).astype(jnp.bfloat16)
        part = matmul(upper, mine)
        same_far = send(edge[border:], lambda s, p: (far(s), p))
        same_near = send(edge[:border], lambda s, p: (near(s), p))
        if build:
            next_coupling()
            swapped, coupling[-1] = meet(swapped, coupling[-1])
        return part, swapped, same_near, cross_near, same_far, cross_far

    copies = lax.axis_size("sub")

    def exchange(values):
        return lax.all_to_all(values, "sub", 0, 0)

    diagonal = []
    vector = jax.ShapeDtypeStruct((own, cols), jnp.float32)
    panel_rows = jax.ShapeDtypeStruct((half, cols), jnp.bfloat16)
    sums = jnp.stack([jnp.sum(shadow * residual, axis=0), jnp.sum(shadow * shadow, axis=0)])
    sums = jnp.broadcast_to(sums[None], (copies, 2, cols))
    sums, lists = lax.optimization_barrier((sums, send_rows))
    near_far = [by_parity(lists[0, 1], lists[0, 0]), by_parity(lists[0, 0], lists[0, 1])]
    select = (jnp.concatenate(near_far)[:, None] == rows).astype(jnp.bfloat16)
    chosen_upper = matmul(select, upper).astype(jnp.bfloat16)
    opening_sums, chosen_upper = meet(exchange(sums), chosen_upper)
    past = jnp.stack([rho_prev, alpha_prev, omega_prev])
    opening, mine, payload = small_call(
        lambda *refs: direction_kernel(node_count, *refs),
        panel,
        (opening_sums, past, residual, direction, old_image, select),
        [jax.ShapeDtypeStruct((2, cols), jnp.float32), panel_rows, panel_rows],
    )
    parts = precondition(mine, payload, True)
    direction_hat, image_new, sums = operate(parts, diagonal[0], shadow, None, coupling, copies)
    step_alpha, middle, mine, payload = small_call(
        lambda *refs: middle_kernel(node_count, *refs),
        panel,
        (exchange(sums), opening, residual, image_new, select),
        [jax.ShapeDtypeStruct((1, cols), jnp.float32), vector, panel_rows, panel_rows],
    )
    step_alpha = step_alpha[0]
    parts = precondition(mine, payload, False)
    middle_hat, tested, sums = operate(parts, diagonal[0], shadow, middle, coupling, copies)
    closing = jnp.sum(exchange(sums), axis=0) / node_count
    step_omega = closing[0] / (closing[1] + EPSILON)
    next_rho = closing[2] - step_omega * closing[3]
    new_residual = middle - step_omega * tested
    new_solution = solution + step_alpha * direction_hat + step_omega * middle_hat
    return (new_solution, new_residual, step_alpha, step_omega, next_rho)


def solution(mesh):
    assert mesh.shape["panel"] == 2 and mesh.shape["sub"] % 2 == 0
    placed = (
        P("sub", "panel"),
        P("sub", "panel"),
        P("sub", "panel"),
        P("sub", "panel"),
        P("sub", "panel"),
        P("panel"),
        P("panel"),
        P("panel"),
        P("sub", None, "panel"),
        P("sub", None, "panel"),
        P(None, "sub"),
        P(None, "sub"),
        P("sub"),
        P("sub", None, None),
    )
    return jax.shard_map(
        per_device,
        mesh=mesh,
        in_specs=placed,
        out_specs=(P("sub", "panel"), P("sub", "panel"), P("panel"), P("panel"), P("panel")),
        check_vma=False,
    )
```

```python
import jax
import jax.numpy as jnp
from jax import lax
from jax.experimental import pallas as pl
from jax.experimental.pallas import tpu as pltpu
from jax.sharding import PartitionSpec as P

FLOOR_SHARE = 0.3
EPSILON = 1e-06
AXES = ("sub", "panel")


def send(values, route):
    subs = lax.axis_size("sub")
    panels = lax.axis_size("panel")
    pairs = []
    for s in range(subs):
        for p in range(panels):
            target = route(s, p)
            if target is not None:
                pairs.append((s * panels + p, (target[0] % subs) * panels + target[1]))
    return lax.ppermute(values, AXES, pairs)


def merge_repeated(links, weights):
    merged = []
    for k in range(links.shape[0]):
        total = weights[k : k + 1]
        for j in range(k):
            total += jnp.where(links[j : j + 1] == links[k : k + 1], weights[j : j + 1], 0.0)
        merged.append(total)
    return jnp.concatenate(merged, axis=0)


def coupling_kernel(neighbours_ref, weight_ref, out_ref, link_rows, weight_rows):
    links = neighbours_ref[...]
    link_rows[...] = links.T
    weight_rows[...] = merge_repeated(links, weight_ref[...]).T
    group, lanes = 16, 128
    shape = (group, out_ref.shape[1])
    repeats = shape[1] // lanes
    columns = lax.broadcasted_iota(jnp.int32, shape, 1).astype(jnp.int16)

    def body(index, carry):
        rows = pl.ds(index * group, group)
        links, weights = link_rows[rows, :], weight_rows[rows, :]
        total = jnp.zeros(shape, jnp.bfloat16)
        for k in range(links.shape[1]):
            link = jnp.broadcast_to(links[:, k : k + 1], (group, lanes)).astype(jnp.int16)
            weight = jnp.broadcast_to(weights[:, k : k + 1], (group, lanes)).astype(jnp.bfloat16)
            hit = jnp.concatenate([link] * repeats, axis=1) == columns
            total = jnp.where(hit, jnp.concatenate([weight] * repeats, axis=1), total)
        out_ref[rows, :] = total
        return carry

    lax.fori_loop(0, out_ref.shape[0] // group, body, 0, unroll=4)


def coupling_rows(neighbours, edge_weight, ext, begin, count):
    slots = neighbours.shape[0]
    rows = 128
    return pl.pallas_call(
        coupling_kernel,
        grid=(count,),
        in_specs=[pl.BlockSpec((slots, rows), lambda i: (0, i + begin))] * 2,
        out_specs=pl.BlockSpec((rows, ext), lambda i: (i, 0)),
        out_shape=jax.ShapeDtypeStruct((rows * count, ext), jnp.bfloat16),
        scratch_shapes=[
            pltpu.VMEM((rows, slots), jnp.int32),
            pltpu.VMEM((rows, slots), jnp.float32),
        ],
        cost_estimate=pl.CostEstimate(
            flops=50 * slots * rows * count * ext,
            bytes_accessed=2 * rows * count * ext,
            transcendentals=0,
        ),
        compiler_params=pltpu.CompilerParams(vmem_limit_bytes=8 << 20),
    )(neighbours, edge_weight)


def operate_kernel(closing, *refs):
    part, swapped, same_near, cross_near, same_far, cross_far, diagonal, shadow = refs[:8]
    refs = refs[8:]
    if closing:
        middle, refs = refs[0], refs[1:]
    *weights, hat_out, image_out, sums_ref, extended, hat_ref, image_ref, done = refs
    own, border = part.shape[0], same_near.shape[0]
    hat = part[...] + swapped[...].astype(jnp.float32)
    hat_ref[...] = hat
    extended[:own] = hat.astype(jnp.bfloat16)
    for at, (same, cross) in enumerate(((same_near, cross_near), (same_far, cross_far))):
        ghost = same[...].astype(jnp.float32) + cross[...].astype(jnp.float32)
        extended[own + at * border : own + (at + 1) * border] = ghost.astype(jnp.bfloat16)
    begin = 0
    sums = 0.0
    leaving = [pltpu.make_async_copy(hat_ref, hat_out, done.at[0])]
    leaving[0].start()
    for weight in weights:
        rows = slice(begin, begin + weight.shape[0])
        begin += weight.shape[0]
        coupled = jnp.dot(weight[...], extended[...], preferred_element_type=jnp.float32)
        image = diagonal[rows] * hat_ref[rows] - coupled
        image_ref[rows] = image
        leaving.append(
            pltpu.make_async_copy(image_ref.at[rows], image_out.at[rows], done.at[len(leaving)])
        )
        leaving[-1].start()
        if closing:
            pairs = (
                (image, middle[rows]),
                (image, image),
                (shadow[rows], middle[rows]),
                (shadow[rows], image),
            )
        else:
            pairs = ((shadow[rows], image), (image, image))
        sums += jnp.concatenate([jnp.sum(a * b, axis=0, keepdims=True) for a, b in pairs], axis=0)
    sums_ref[...] = jnp.broadcast_to(sums[None], sums_ref.shape)
    for copy in leaving:
        copy.wait()


def operate(parts, diagonal, shadow, middle, coupling, copies):
    closing = middle is not None
    operands = [*parts, diagonal, shadow] + ([middle] if closing else []) + list(coupling)
    own, cols = shadow.shape
    vector = jax.ShapeDtypeStruct((own, cols), jnp.float32)
    count = 4 if closing else 2
    ext = coupling[0].shape[1]
    in_vmem = pl.BlockSpec(memory_space=pltpu.VMEM)
    return pl.pallas_call(
        lambda *refs: operate_kernel(closing, *refs),
        in_specs=[in_vmem] * len(operands),
        out_specs=[pl.BlockSpec(memory_space=pltpu.HBM)] * 2 + [in_vmem],
        out_shape=[vector, vector, jax.ShapeDtypeStruct((copies, count, cols), jnp.float32)],
        scratch_shapes=[
            pltpu.VMEM((ext, cols), jnp.bfloat16),
            pltpu.VMEM((own, cols), jnp.float32),
            pltpu.VMEM((own, cols), jnp.float32),
            pltpu.SemaphoreType.DMA((1 + len(coupling),)),
        ],
        cost_estimate=pl.CostEstimate(
            flops=2 * own * ext * cols, bytes_accessed=2 * own * ext, transcendentals=0
        ),
        compiler_params=pltpu.CompilerParams(vmem_limit_bytes=24 << 20),
        name="operate_closing" if closing else "operate_second",
    )(*operands)


def split_rows(vector, select, panel, mine_ref, payload_ref):
    rounded = vector.astype(jnp.bfloat16)
    half = mine_ref.shape[0]
    tail = rounded.shape[0] - half
    ghosts = jnp.dot(select[...], rounded, preferred_element_type=jnp.float32)
    ghosts = ghosts.astype(jnp.bfloat16)

    def put(head_ref, rest_ref):
        head_ref[...] = rounded[:half]
        rest_ref[:tail] = rounded[half:]
        rest_ref[tail:] = ghosts

    pl.when(panel[0] == 0)(lambda: put(mine_ref, payload_ref))
    pl.when(panel[0] != 0)(lambda: put(payload_ref, mine_ref))


def direction_kernel(node_count, panel, sums, past, residual, direction, old_image, select, *outs):
    means_ref, mine_ref, payload_ref = outs
    means = jnp.sum(sums[...], axis=0) / node_count
    means_ref[...] = means
    rho_prev, alpha_prev, omega_prev = past[0:1], past[1:2], past[2:3]
    step_beta = means[0:1] / rho_prev * (alpha_prev / omega_prev)
    vector = residual[...] + step_beta * (direction[...] - omega_prev * old_image[...])
    split_rows(vector, select, panel, mine_ref, payload_ref)


def middle_kernel(node_count, panel, sums, opening, residual, image, select, *outs):
    alpha_ref, middle_ref, mine_ref, payload_ref = outs
    means = jnp.sum(sums[...], axis=0) / node_count
    floor = FLOOR_SHARE * jnp.sqrt(opening[1:2] * means[1:2])
    step_alpha = opening[0:1] / jnp.maximum(means[0:1], floor)
    alpha_ref[...] = step_alpha
    middle = residual[...] - step_alpha * image[...]
    middle_ref[...] = middle
    split_rows(middle, select, panel, mine_ref, payload_ref)


def small_call(kernel, panel, operands, outs):
    in_vmem = pl.BlockSpec(memory_space=pltpu.VMEM)
    return pl.pallas_call(
        kernel,
        in_specs=[pl.BlockSpec(memory_space=pltpu.SMEM)] + [in_vmem] * len(operands),
        out_specs=[in_vmem] * len(outs),
        out_shape=outs,
        compiler_params=pltpu.CompilerParams(vmem_limit_bytes=12 << 20),
    )(panel.reshape(1), *operands)


def near(s):
    return s ^ 1


def far(s):
    return s - 1 if s % 2 == 0 else s + 1


def matmul(left, right):
    return jnp.dot(left, right, preferred_element_type=jnp.float32)


def per_device(
    solution,
    residual,
    shadow,
    direction,
    old_image,
    rho_prev,
    alpha_prev,
    omega_prev,
    lower_inverse,
    upper_inverse,
    neighbours,
    edge_weight,
    node_shift,
    send_rows,
):
    panel = lax.axis_index("panel")
    first = panel == 0
    own, cols = residual.shape
    node_count = own * lax.axis_size("sub")
    lower = lower_inverse[0]
    ext, half = lower.shape
    upper = upper_inverse[0, :own]
    border = send_rows.shape[2]
    tail = own - half

    blocks = own // 128
    cuts = (0, blocks // 2, blocks)
    coupling = []

    def next_coupling():
        begin, end = cuts[len(coupling) : len(coupling) + 2]
        coupling.append(coupling_rows(neighbours, edge_weight, ext, begin, end - begin))

    def meet(arrived, value):
        return lax.optimization_barrier((arrived, value))

    even = lax.axis_index("sub") % 2 == 0

    def by_parity(zero, one):
        return jnp.where(even, zero, one)

    turned = jnp.where(neighbours < own + border, neighbours + border, neighbours - border)
    ghost = even & (neighbours >= own) & (neighbours < ext)
    neighbours = jnp.where(ghost, turned, neighbours)
    rows = lax.broadcasted_iota(jnp.int32, (1, own), 1)

    def by_panel(zero, one):
        return jnp.where(first, zero, one)

    diagonal_rows = lax.dynamic_slice_in_dim(lower, panel * half, half, axis=0)

    def precondition(mine, payload, chosen_upper):
        build = chosen_upper is None
        received = send(payload, lambda s, p: (s, 1 - p))
        early = matmul(lower[half:], mine).astype(jnp.bfloat16)
        passed_others = send(early, lambda s, p: (s, 1) if p == 0 else None)
        if build:
            next_coupling()
            received, coupling[-1] = meet(received, coupling[-1])
        near_rows, far_rows = slice(tail, tail + border), slice(tail + border, half)

        def both(part):
            return jnp.concatenate([received[part], mine[part]], axis=1)

        from_far = send(both(far_rows), lambda s, p: (far(s), 1) if p == 1 else None)
        from_near = send(both(near_rows), lambda s, p: (near(s), 1) if p == 1 else None)
        late = matmul(lower[half:], received).astype(jnp.bfloat16)
        if build:
            late, chosen = lax.optimization_barrier((late, select))
            chosen_upper = matmul(chosen, upper).astype(jnp.bfloat16)
        passed_mine = send(late, lambda s, p: (s, 1) if p == 0 else None)
        if build:
            from_far, chosen_upper = meet(from_far, chosen_upper)
        from_lower, from_upper = by_parity(from_far, from_near), by_parity(from_near, from_far)

        def solve(kept, ghost_columns, passed):
            ghosts = [from_lower[:, ghost_columns], from_upper[:, ghost_columns]]
            rhs = by_panel(kept, jnp.concatenate([kept[:tail], *ghosts], axis=0))
            product = matmul(diagonal_rows, rhs) + passed.astype(jnp.float32)
            return lax.optimization_barrier(product.astype(jnp.bfloat16))

        others = solve(received, slice(0, cols), passed_others)
        if build:
            others, links = lax.optimization_barrier((others, neighbours))
            present = jnp.where(links < ext, edge_weight, 0.0)
            scale = jnp.broadcast_to((node_shift + jnp.sum(present, axis=0))[:, None], (own, cols))
            diagonal.append(scale)
        other_part = matmul(upper, others).astype(jnp.bfloat16)
        swapped = send(other_part, lambda s, p: (s, 1 - p))
        other_edge = matmul(chosen_upper, others).astype(jnp.bfloat16)
        cross_far = send(other_edge[border:], lambda s, p: (far(s), 1 - p))
        cross_near = send(other_edge[:border], lambda s, p: (near(s), 1 - p))
        mine = solve(mine, slice(cols, 2 * cols), passed_mine)
        edge = matmul(chosen_upper, mine).astype(jnp.bfloat16)
        part = matmul(upper, mine)
        same_far = send(edge[border:], lambda s, p: (far(s), p))
        same_near = send(edge[:border], lambda s, p: (near(s), p))
        if build:
            next_coupling()
            swapped, coupling[-1] = meet(swapped, coupling[-1])
        return (part, swapped, same_near, cross_near, same_far, cross_far), chosen_upper

    copies = lax.axis_size("sub")

    def exchange(values):
        return lax.all_to_all(values, "sub", 0, 0)

    diagonal = []
    vector = jax.ShapeDtypeStruct((own, cols), jnp.float32)
    panel_rows = jax.ShapeDtypeStruct((half, cols), jnp.bfloat16)
    sums = jnp.stack([jnp.sum(shadow * residual, axis=0), jnp.sum(shadow * shadow, axis=0)])
    sums = jnp.broadcast_to(sums[None], (copies, 2, cols))
    sums, lists = lax.optimization_barrier((sums, send_rows))
    near_far = [by_parity(lists[0, 1], lists[0, 0]), by_parity(lists[0, 0], lists[0, 1])]
    select = (jnp.concatenate(near_far)[:, None] == rows).astype(jnp.bfloat16)
    past = jnp.stack([rho_prev, alpha_prev, omega_prev])
    opening, mine, payload = small_call(
        lambda *refs: direction_kernel(node_count, *refs),
        panel,
        (exchange(sums), past, residual, direction, old_image, select),
        [jax.ShapeDtypeStruct((2, cols), jnp.float32), panel_rows, panel_rows],
    )
    parts, chosen_upper = precondition(mine, payload, None)
    direction_hat, image_new, sums = operate(parts, diagonal[0], shadow, None, coupling, copies)
    step_alpha, middle, mine, payload = small_call(
        lambda *refs: middle_kernel(node_count, *refs),
        panel,
        (exchange(sums), opening, residual, image_new, select),
        [jax.ShapeDtypeStruct((1, cols), jnp.float32), vector, panel_rows, panel_rows],
    )
    step_alpha = step_alpha[0]
    parts, _ = precondition(mine, payload, chosen_upper)
    middle_hat, tested, sums = operate(parts, diagonal[0], shadow, middle, coupling, copies)
    closing = jnp.sum(exchange(sums), axis=0) / node_count
    step_omega = closing[0] / (closing[1] + EPSILON)
    next_rho = closing[2] - step_omega * closing[3]
    new_residual = middle - step_omega * tested
    new_solution = solution + step_alpha * direction_hat + step_omega * middle_hat
    return (new_solution, new_residual, step_alpha, step_omega, next_rho)


def solution(mesh):
    assert mesh.shape["panel"] == 2 and mesh.shape["sub"] % 2 == 0
    placed = (
        P("sub", "panel"),
        P("sub", "panel"),
        P("sub", "panel"),
        P("sub", "panel"),
        P("sub", "panel"),
        P("panel"),
        P("panel"),
        P("panel"),
        P("sub", None, "panel"),
        P("sub", None, "panel"),
        P(None, "sub"),
        P(None, "sub"),
        P("sub"),
        P("sub", None, None),
    )
    return jax.shard_map(
        per_device,
        mesh=mesh,
        in_specs=placed,
        out_specs=(P("sub", "panel"), P("sub", "panel"), P("panel"), P("panel"), P("panel")),
        check_vma=False,
    )
```
